256 devices in a mesh: ctx: 32 (over z, x_hi, core), head: 8 (over y, x_lo).
Axes of the slice: x: 4 (x_hi: 2, x_lo: 2; x = x_hi * 2 + x_lo), y: 4, z: 8, core: 2. Of those that a mesh axis runs over, the one named last changes fastest.
Arguments:
- query_heads: bfloat16 [8192, 32, 128], P('ctx', 'head'), may hold values from -5 to 5
- key_heads: bfloat16 [8192, 16, 128], P('ctx', 'head'), may hold values from -5 to 5
- value_heads: bfloat16 [8192, 16, 128], P('ctx', 'head'), may hold values from -6 to 6
- positions: int32 [8192], P('ctx'), may hold values from 0 to 8191, each once
- out_weight: bfloat16 [4096, 4608], P('head'), may hold values from -0.125 to 0.125
Outputs:
- attn_out: bfloat16 [8192, 4608], P('ctx', 'head')
The draws below stay inside these ranges and needn't reach their ends.
Inputs may be any that keep to these rules, and one draw needn't show every extreme that they name: Each of the 8192 positions appears exactly once.
All inputs are finite; a program needn't handle non-finite values.
Results may differ from the reference program's by a relative error of at most 0.0081.
Values may be sent and summed in bfloat16 or wider, within the bound.
A program may use at most 64 MiB of HBM per device.

```python
import jax
import jax.numpy as jnp
from jax import lax

D = 4608
HEADS = 32
KV = 16
HD = 128
SEQ = 8192


def base_values(key, shape, spread):
    values = jax.random.normal(jax.random.fold_in(key, 5), shape, jnp.float32) * spread
    return jnp.clip(values, -5.0, 5.0)


def draw_query_heads(key, part):
    values = base_values(jax.random.fold_in(key, 1), (SEQ, HEADS, HD), 1.5)
    return values.astype(jnp.bfloat16)


def draw_key_heads(key, part):
    values = base_values(jax.random.fold_in(key, 2), (SEQ, KV, HD), 1.0)
    return values.astype(jnp.bfloat16)


def with_spikes(result, stream_key, source, target, blocks, factor):
    owner, partner = [(jnp.arange(result.shape[axis_at]) // (result.shape[axis_at] // blocks)).reshape([-1 if axis == axis_at else 1 for axis in range(result.ndim)]) for axis_at in (source, target)]
    chosen = jax.random.permutation(stream_key, blocks)[partner]
    strong = (owner == chosen) | (owner == (partner + blocks // 2) % blocks)
    return jnp.where(strong, factor * result, result)


def shard_levels(stream_key, extent, shards, least, top_value):
    factor_of, own = 1.0, jax.random.fold_in(stream_key, 6)
    for dim, blocks in shards:
        draws = jnp.exp(jax.random.uniform(jax.random.fold_in(own, dim), (blocks,), jnp.float32, least / len(shards), top_value / len(shards)))
        factor_of = factor_of * jnp.repeat(draws, extent[dim] // blocks).reshape([-1 if axis == dim else 1 for axis in range(len(extent))])
    return factor_of


def normal_values(stream_key, shape, scale, bound, pieces=(), kind=jnp.bfloat16):
    array = jax.random.normal(stream_key, shape, jnp.float32) * scale
    if len(pieces) > 0:
        array = shard_levels(stream_key, shape, pieces, -0.22, 0.18) * array
    return jnp.clip(array, min=-bound, max=bound).astype(kind)


def bell_draw_with(own_key, shape, scale, reach, pieces, heavy, held_as=jnp.bfloat16):
    result = scale * jax.random.normal(own_key, shape, jnp.float32)
    if pieces:
        result = result * shard_levels(own_key, shape, pieces, -0.22, 0.18)
    return jnp.clip(with_spikes(result, jax.random.fold_in(own_key, 3), *heavy), -reach, reach).astype(held_as)


def setup_inputs(seed: int = 0) -> dict:
    arg_keys = jax.random.split(jax.random.key(seed), 6)
    query_heads = draw_query_heads(jax.random.fold_in(arg_keys[5], 71), 0)
    key_heads = draw_key_heads(jax.random.fold_in(arg_keys[5], 71), 0)
    value_heads = normal_values(arg_keys[2], (SEQ, KV, HD), 1.0, 6.0, ((0, 32), (1, 8)))
    positions = jax.random.permutation(arg_keys[3], SEQ).astype(jnp.int32)
    out_weight = bell_draw_with(arg_keys[4], (HEADS * HD, D), (HEADS * HD) ** -0.5, 0.125, ((0, 8),), (0, 1, 8, 2.0))
    return dict(query_heads=query_heads, key_heads=key_heads, value_heads=value_heads, positions=positions, out_weight=out_weight)


NEG_BIG = -1.0e30
ATTN_SCALE = 1.0 / 12.0


def reference(query_heads, key_heads, value_heads, positions, out_weight):
    group_size = HEADS // KV
    visible = positions[None, :] <= positions[:, None]

    def one_head(head_index):
        query_one = lax.dynamic_index_in_dim(query_heads, head_index, 1, keepdims=False)
        kv_index = (head_index // group_size).astype(jnp.int32)
        key_one = lax.dynamic_index_in_dim(key_heads, kv_index, 1, keepdims=False)
        value_one = lax.dynamic_index_in_dim(value_heads, kv_index, 1, keepdims=False)
        scores = jnp.dot(query_one, key_one.T, preferred_element_type=jnp.float32) * ATTN_SCALE
        scores = jnp.where(visible, scores, NEG_BIG)
        row_max = jnp.max(scores, axis=1)
        weights = jnp.where(visible, jnp.exp(scores - row_max[:, None]), 0.0)
        denom = jnp.sum(weights, axis=1)
        summed = jnp.dot(weights.astype(jnp.bfloat16), value_one, preferred_element_type=jnp.float32)
        return (summed / denom[:, None]).astype(jnp.bfloat16)

    attended = lax.map(one_head, jnp.arange(HEADS, dtype=jnp.int32))
    flat = jnp.transpose(attended, (1, 0, 2)).reshape(SEQ, HEADS * HD)
    return jnp.dot(flat, out_weight, preferred_element_type=jnp.float32).astype(jnp.bfloat16)
```

```python
import jax
import jax.numpy as jnp
from jax import lax
from jax.experimental import pallas as pl
from jax.experimental.pallas import tpu as pltpu
from jax.sharding import PartitionSpec as P

MESH = pl.DeviceIdType.MESH
NEG_BIG = -1e30
LOG2E = 1.4426950408889634
SCALE = LOG2E / 12.0
NZ = 8
TOK = 256
QUART = 128
HD = 128
STEPS = NZ
STEP_KEYS = 512
ROWS = 512
PAIR = 1152
OUT = 576
XCOLS = 640
F32 = jnp.float32
BF16 = jnp.bfloat16


def kernel(
    q_ref, kv_ref, pos_ref, w_hbm, out_ref,
    kvb, posb, qb, qpos, kb, vtb, pkb, acc, mrun, lrun,
    stage, lstage, attp, lsep, att, w_ref,
    tb, tf, ra, rb, sumf, xs, xr,
    s_kv1, s_kvf, s_pos1, s_posf, s_loc, s_q, s_qp, s_o, s_l, s_a, s_b, s_x,
    r_kv, r_pos, r_q, r_qp, r_o, r_l, r_a, r_b, r_x, w_sem,
):
    ctx, head = lax.axis_index("ctx"), lax.axis_index("head")
    core, xh, z = ctx % 2, (ctx // 2) % 2, ctx // 4
    y, xl = head // 2, head % 2
    other = 1 - core

    def at(zz, xx, cc):
        return ((zz * 2 + xx) * 2 + cc, head)

    z_up, z_down = (z + 1) % NZ, (z + NZ - 1) % NZ
    partner = at(z, xh, other)
    y_up, y_down = (ctx, ((y + 1) % 4) * 2 + xl), (ctx, ((y + 3) % 4) * 2 + xl)
    x_pair = (ctx, y * 2 + 1 - xl)
    peers = [partner, y_up, y_down, x_pair]
    for cc in range(2):
        peers += [at(z_up, xh, cc), at(z_down, xh, cc), at(z, 1 - xh, cc)]
    barrier = pltpu.get_barrier_semaphore()
    for peer in peers:
        pl.semaphore_signal(barrier, inc=1, device_id=peer, device_id_type=MESH)

    w_copy = pltpu.make_async_copy(w_hbm, w_ref, w_sem)
    w_copy.start()

    def remote(src, dst, ssem, rsem, dev):
        return pltpu.make_async_remote_copy(
            src_ref=src, dst_ref=dst, send_sem=ssem, recv_sem=rsem,
            device_id=dev, device_id_type=MESH,
        )

    def kv_own(j, h):
        return kv_ref.at[pl.ds(j * QUART, QUART), pl.ds(h * 256, 256)]

    pl.semaphore_wait(barrier, len(peers))

    own_half = z * 2 + core
    sends = []

    def start(copy):
        copy.start()
        sends.append(copy)

    for j in range(2):
        slot = z * 4 + core * 2 + j
        for h in range(2):
            for d, zz in enumerate((z_up, z_down)):
                if j == 0:
                    start(remote(pos_ref, posb.at[own_half], s_pos1.at[d, h], r_pos.at[own_half], at(zz, xh, h)))
                start(remote(kv_own(j, h), kvb.at[slot], s_kv1.at[d, h, j], r_kv.at[slot], at(zz, xh, h)))
    start(remote(pos_ref, posb.at[own_half], s_pos1.at[2, 0], r_pos.at[own_half], partner))
    for j in range(2):
        slot = z * 4 + core * 2 + j
        lane = pl.multiple_of(other * 256, 256)
        start(remote(kv_ref.at[pl.ds(j * QUART, QUART), pl.ds(lane, 256)], kvb.at[slot], s_loc.at[j], r_kv.at[slot], partner))
    lane = pl.multiple_of(other * 256, 256)
    start(remote(q_ref.at[:, pl.ds(lane, 256)], qb.at[2 + core], s_q.at[2], r_q.at[2 + core], partner))
    start(remote(pos_ref, qpos.at[2 + core], s_qp.at[2], r_qp.at[2 + core], partner))
    for h in range(2):
        dev = at(z, 1 - xh, h)
        start(remote(q_ref.at[:, pl.ds(h * 256, 256)], qb.at[core], s_q.at[h], r_q.at[core], dev))
        start(remote(pos_ref, qpos.at[core], s_qp.at[h], r_qp.at[core], dev))

    lane = pl.multiple_of(core * 256, 256)
    qb[2 + core] = q_ref[:, pl.ds(lane, 256)]
    qpos[2 + core] = pos_ref[...]
    posb[own_half] = pos_ref[...]
    for j in range(2):
        kvb[z * 4 + core * 2 + j] = kv_ref[pl.ds(j * QUART, QUART), pl.ds(lane, 256)]

    mrun[...] = jnp.full(mrun.shape, NEG_BIG, F32)
    lrun[...] = jnp.zeros(lrun.shape, F32)
    acc[...] = jnp.zeros(acc.shape, F32)

    def arrived(step, at_quarter, slot):
        rows = pl.ds(pl.multiple_of(at_quarter * QUART, QUART), QUART)
        kb[step, rows, :] = kvb[slot, :, :HD]
        vtb[step, :, rows] = kvb[slot, :, HD:].T
        lanes = pl.ds(pl.multiple_of((slot % 2) * QUART, QUART), QUART)
        line = posb[slot // 2, :, lanes]
        pkb[step, rows, :] = jnp.broadcast_to(line, (QUART, QUART)).T

    def wait_pos(half):
        remote(posb.at[half], posb.at[half], s_pos1.at[0, 0], r_pos.at[half], partner).wait_recv()

    def wait_kv(slot):
        remote(kvb.at[slot], kvb.at[slot], s_kv1.at[0, 0, 0], r_kv.at[slot], partner).wait_recv()

    for j in range(2):
        arrived(0, core * 2 + j, z * 4 + core * 2 + j)
    wait_pos(z * 2 + other)
    for j in range(2):
        slot = z * 4 + other * 2 + j
        wait_kv(slot)
        arrived(0, other * 2 + j, slot)
    remote(qb.at[2 + other], qb.at[2 + other], s_q.at[0], r_q.at[2 + other], partner).wait_recv()
    remote(qpos.at[2 + other], qpos.at[2 + other], s_qp.at[0], r_qp.at[2 + other], partner).wait_recv()

    def service(i):
        hop, a = i // 4 + 1, i % 4
        step = i // 2 + 1
        for d in range(2):
            src_z = (z + NZ - hop) % NZ if d == 0 else (z + hop) % NZ
            quarter = a if d == 0 else (a + 2) % 4
            slot = src_z * 4 + quarter
            half = slot // 2
            dev = at(z_up if d == 0 else z_down, xh, core)

            @pl.when(a % 2 == 0)
            def _():
                wait_pos(half)

                @pl.when(i < 10)
                def _():
                    remote(posb.at[half], posb.at[half], s_posf.at[d, i // 2], r_pos.at[half], dev).start()

            wait_kv(slot)

            @pl.when(i < 10)
            def _():
                remote(kvb.at[slot], kvb.at[slot], s_kvf.at[d, i], r_kv.at[slot], dev).start()

            arrived(step, (i % 2) * 2 + d, slot)

    def unit(step, g):
        k = kb[step]
        vt = vtb[step]
        pk = pkb[step]
        line = qpos[g]
        mask = jnp.concatenate([pk, pk], axis=1) <= line
        for h in range(2):
            cols = slice(h * TOK, (h + 1) * TOK)
            q = qb[g, :, h * HD:(h + 1) * HD]
            s = lax.dot_general(k, q, (((1,), (1,)), ((), ())), preferred_element_type=F32)
            s = jnp.where(mask, s * SCALE, NEG_BIG)
            m_old = mrun[g, :, cols]
            m_new = jnp.maximum(m_old, jnp.max(s, axis=0, keepdims=True))
            p = jnp.exp2(s - m_new)
            alpha = jnp.exp2(m_old - m_new)
            part = jnp.sum(p.reshape(STEP_KEYS // 8, 8, TOK), axis=0)
            lrun[g, :, cols] = lrun[g, :, cols] * alpha + part
            mrun[g, :, cols] = m_new
            add = jnp.dot(vt, p.astype(BF16), preferred_element_type=F32)
            acc[g, :, cols] = acc[g, :, cols] * alpha + add

    def finalize(g):
        total = jnp.sum(lrun[g], axis=0, keepdims=True)
        lse = mrun[g] + jnp.log2(total)
        o = (acc[g] * (1.0 / total)).astype(BF16)

        @pl.when(g == 2 + core)
        def _():
            attp[0, core] = o
            lsep[0, core] = lse

        @pl.when(g != 2 + core)
        def _():
            stage[g] = o
            lstage[g] = lse

        @pl.when(g < 2)
        def _():
            dev = at(z, 1 - xh, g)
            remote(stage.at[g], attp.at[1, core], s_o.at[g], r_o.at[1, core], dev).start()
            remote(lstage.at[g], lsep.at[1, core], s_l.at[g], r_l.at[1, core], dev).start()

        @pl.when(g == 2 + other)
        def _():
            remote(stage.at[g], attp.at[0, core], s_o.at[2], r_o.at[0, core], partner).start()
            remote(lstage.at[g], lsep.at[0, core], s_l.at[2], r_l.at[0, core], partner).start()

    def body(u, carry):
        early = u < 8
        r = jnp.maximum(u - 8, 0)
        it, w = r // 6, r % 6
        own_g = jnp.where(u % 2 == 0, 2 + other, 2 + core)
        step = jnp.where(early, u // 2, jnp.where(w < 4, 2 * it + w // 2, 4 + it))
        g = jnp.where(early | (w >= 4), own_g, w % 2)

        @pl.when((u >= 1) & early)
        def _():
            service(u - 1)

        @pl.when((u >= 10) & (u <= 28) & ((u - 10) % 3 == 0))
        def _():
            service(7 + (u - 10) // 3)

        @pl.when(u == 8)
        def _():
            for gg in range(2):
                remote(qb.at[gg], qb.at[gg], s_q.at[0], r_q.at[gg], partner).wait_recv()
                remote(qpos.at[gg], qpos.at[gg], s_qp.at[0], r_qp.at[gg], partner).wait_recv()

        unit(step, g)

        @pl.when(u >= 28)
        def _():
            finalize(g)

        return carry

    lax.fori_loop(0, 32, body, 0)

    def wait_part(p, h):
        remote(attp.at[p, h], attp.at[p, h], s_o.at[0], r_o.at[p, h], partner).wait_recv()
        remote(lsep.at[p, h], lsep.at[p, h], s_l.at[0], r_l.at[p, h], partner).wait_recv()

    wait_part(0, other)
    w_copy.wait()
    for h in range(2):
        wait_part(1, h)
        a, b = lsep[0, h], lsep[1, h]
        top = jnp.maximum(a, b)
        wa, wb = jnp.exp2(a - top), jnp.exp2(b - top)
        inv = 1.0 / (wa + wb)
        o = attp[0, h].astype(F32) * (wa * inv) + attp[1, h].astype(F32) * (wb * inv)
        o = o.astype(BF16)
        for hh in range(2):
            lo = (2 * h + hh) * HD
            att[:, lo:lo + HD] = o[:, hh * TOK:(hh + 1) * TOK].T

    def terms(rel, rows):
        cols = pl.ds(pl.multiple_of(((y + rel) % 4) * PAIR, 128), PAIR)
        return jnp.dot(att[rows, :], w_ref[:, cols], preferred_element_type=F32)

    low, high = slice(0, 128), slice(128, 256)
    lo_d, hi_d = pl.ds(0, 128), pl.ds(128, 128)
    tb[1, low, :] = terms(2, low).astype(BF16)
    start(remote(tb.at[1, lo_d], ra.at[0], s_a.at[0], r_a.at[0], y_up))
    tb[1, high, :] = terms(2, high).astype(BF16)
    start(remote(tb.at[1, hi_d], ra.at[1], s_a.at[1], r_a.at[1], y_down))
    tb[0, high, :] = terms(1, high).astype(BF16)
    start(remote(tb.at[0, hi_d], rb.at[0, hi_d], s_b.at[0, 1], r_b.at[0, 1], y_up))
    tb[2, low, :] = terms(3, low).astype(BF16)
    start(remote(tb.at[2, lo_d], rb.at[1, lo_d], s_b.at[1, 0], r_b.at[1, 0], y_down))
    tf[0] = terms(1, low)
    tf[1] = terms(3, high)
    remote(ra.at[0], ra.at[0], s_a.at[0], r_a.at[0], y_down).wait_recv()
    tb[0, low, :] = (tf[0] + ra[0].astype(F32)).astype(BF16)
    start(remote(tb.at[0, lo_d], rb.at[0, lo_d], s_b.at[0, 0], r_b.at[0, 0], y_up))
    remote(ra.at[1], ra.at[1], s_a.at[1], r_a.at[1], y_up).wait_recv()
    tb[2, high, :] = (tf[1] + ra[1].astype(F32)).astype(BF16)
    start(remote(tb.at[2, hi_d], rb.at[1, hi_d], s_b.at[1, 1], r_b.at[1, 1], y_down))
    sumf[...] = terms(0, slice(0, 256))
    give = pl.ds(pl.multiple_of((1 - xl) * 512, 512), XCOLS)
    keep = pl.ds(pl.multiple_of(xl * 512, 512), XCOLS)
    for k, rows in enumerate((slice(0, 128), slice(128, 256))):
        for d in range(2):
            piece = rb.at[d, pl.ds(k * 128, 128)]
            remote(piece, piece, s_b.at[0, 0], r_b.at[d, k], y_down).wait_recv()
        full = sumf[rows, :] + rb[0, rows, :].astype(F32) + rb[1, rows, :].astype(F32)
        sumf[rows, :] = full
        xs[k] = sumf[rows, give].astype(BF16)
        start(remote(xs.at[k], xr.at[k], s_x.at[k], r_x.at[k], x_pair))
    for k, rows in enumerate((slice(0, 128), slice(128, 256))):
        remote(xr.at[k], xr.at[k], s_x.at[k], r_x.at[k], x_pair).wait_recv()
        full = sumf[rows, keep] + xr[k].astype(F32)
        out_ref[rows, :] = jnp.where(xl == 1, full[:, 64:], full[:, :OUT]).astype(BF16)

    for copy in sends:
        copy.wait_send()

    def drain(i, carry):
        for d in range(2):
            remote(kvb.at[0], kvb.at[0], s_kvf.at[d, i], r_kv.at[0], partner).wait_send()

            @pl.when(i % 2 == 0)
            def _():
                remote(posb.at[0], posb.at[0], s_posf.at[d, i // 2], r_pos.at[0], partner).wait_send()
        return carry

    lax.fori_loop(0, 10, drain, 0)
    for k in range(3):
        remote(stage.at[0], stage.at[0], s_o.at[k], r_o.at[0, 0], partner).wait_send()
        remote(lstage.at[0], lstage.at[0], s_l.at[k], r_l.at[0, 0], partner).wait_send()


def on_device(query_heads, key_heads, value_heads, positions, out_weight):
    q = query_heads.reshape(TOK, 4 * HD)
    kv = jnp.stack([key_heads, value_heads], axis=2).reshape(TOK, 4 * HD)
    pos = positions.reshape(1, TOK)
    dma = pltpu.SemaphoreType.DMA
    vmem = pl.BlockSpec(memory_space=pltpu.VMEM)
    return pl.pallas_call(
        kernel,
        out_shape=jax.ShapeDtypeStruct((TOK, OUT), BF16),
        in_specs=[vmem, vmem, vmem, pl.BlockSpec(memory_space=pl.ANY)],
        out_specs=vmem,
        scratch_shapes=[
            pltpu.VMEM((4 * NZ, QUART, 2 * HD), BF16),
            pltpu.VMEM((2 * NZ, 1, TOK), jnp.int32),
            pltpu.VMEM((4, TOK, 2 * HD), BF16),
            pltpu.VMEM((4, 1, TOK), jnp.int32),
            pltpu.VMEM((STEPS, STEP_KEYS, HD), BF16),
            pltpu.VMEM((STEPS, HD, STEP_KEYS), BF16),
            pltpu.VMEM((STEPS, STEP_KEYS, QUART), jnp.int32),
            pltpu.VMEM((4, HD, ROWS), F32),
            pltpu.VMEM((4, 1, ROWS), F32),
            pltpu.VMEM((4, 8, ROWS), F32),
            pltpu.VMEM((4, HD, ROWS), BF16),
            pltpu.VMEM((4, 1, ROWS), F32),
            pltpu.VMEM((2, 2, HD, ROWS), BF16),
            pltpu.VMEM((2, 2, 1, ROWS), F32),
            pltpu.VMEM((TOK, 4 * HD), BF16),
            pltpu.VMEM((4 * HD, 4 * PAIR), BF16),
            pltpu.VMEM((3, TOK, PAIR), BF16),
            pltpu.VMEM((2, 128, PAIR), F32),
            pltpu.VMEM((2, 128, PAIR), BF16),
            pltpu.VMEM((2, TOK, PAIR), BF16),
            pltpu.VMEM((TOK, PAIR), F32),
            pltpu.VMEM((2, 128, XCOLS), BF16),
            pltpu.VMEM((2, 128, XCOLS), BF16),
            dma((2, 2, 2)), dma((2, 10)), dma((3, 2)), dma((2, 5)), dma((2,)),
            dma((3,)), dma((3,)), dma((3,)), dma((3,)), dma((2,)), dma((2, 2)), dma((2,)),
            dma((4 * NZ,)), dma((2 * NZ,)), dma((4,)), dma((4,)), dma((2, 2)), dma((2, 2)),
            dma((2,)), dma((2, 2)), dma((2,)), dma,
        ],
        compiler_params=pltpu.CompilerParams(
            collective_id=0, has_side_effects=True, vmem_limit_bytes=60 * 1024 * 1024
        ),
        cost_estimate=pl.CostEstimate(flops=6_000_000_000, bytes_accessed=6_000_000, transcendentals=8_000_000),
    )(q, kv, pos, out_weight)


def solution(mesh):
    return jax.shard_map(
        on_device,
        mesh=mesh,
        in_specs=(
            P("ctx", "head", None),
            P("ctx", "head", None),
            P("ctx", "head", None),
            P("ctx"),
            P("head", None),
        ),
        out_specs=P("ctx", "head"),
        check_vma=False,
    )
```

```python
import jax
import jax.numpy as jnp
from jax import lax
from jax.experimental import pallas as pl
from jax.experimental.pallas import tpu as pltpu
from jax.sharding import PartitionSpec as P

MESH = pl.DeviceIdType.MESH
NEG_BIG = -1e30
LOG2E = 1.4426950408889634
SCALE = LOG2E / 12.0
NZ = 8
TOK = 256
QUART = 128
HD = 128
STEPS = NZ
STEP_KEYS = 512
LANES = 512
OUT = 576
YROWS = 352
XROWS = OUT - YROWS
YCHUNK = YROWS // 2
XHALF = XROWS // 2
F32 = jnp.float32
BF16 = jnp.bfloat16


def kernel(
    q_ref, k_ref, v_ref, pos_ref, w_hbm, out_ref,
    kvs, qs, kvb, posb, qb, qpos, kb, vtb, pkb, acc, mrun, lrun,
    stage, lstage, attp, lsep, att, w_ref, wt,
    tt, ysend, yrecv, xsend, xrecv, dsend, drecv, psend, precv,
    s_kv1, s_kvf, s_pos1, s_posf, s_loc, s_locp, s_q, s_qp, s_o, s_l,
    s_y, s_x, s_d, s_p,
    r_kv, r_pos, r_q, r_qp, r_o, r_l, r_y, r_x, r_d, r_p, w_sem,
):
    ctx, head = lax.axis_index("ctx"), lax.axis_index("head")
    core, xh, z = ctx % 2, (ctx // 2) % 2, ctx // 4
    y, xl = head // 2, head % 2
    other = 1 - core

    def at(zz, xx, cc):
        return ((zz * 2 + xx) * 2 + cc, head)

    z_up, z_down = (z + 1) % NZ, (z + NZ - 1) % NZ
    partner = at(z, xh, other)
    y_next = ((ctx, ((y + 1) % 4) * 2 + xl), (ctx, ((y + 3) % 4) * 2 + xl))
    x_pair = (ctx, y * 2 + 1 - xl)
    peers = [partner, y_next[0], y_next[1], x_pair]
    for cc in range(2):
        peers += [at(z_up, xh, cc), at(z_down, xh, cc), at(z, 1 - xh, cc)]
    barrier = pltpu.get_barrier_semaphore()
    for peer in peers:
        pl.semaphore_signal(barrier, inc=1, device_id=peer, device_id_type=MESH)

    w_copy = pltpu.make_async_copy(w_hbm, w_ref, w_sem)
    w_copy.start()

    for h in range(2):
        kvs[:, h * 256:h * 256 + HD] = k_ref[:, h, :]
        kvs[:, h * 256 + HD:(h + 1) * 256] = v_ref[:, h, :]
        for half in range(2):
            for hh in range(2):
                qs[h, half, hh * 128:(hh + 1) * 128, :] = q_ref[half * 128:(half + 1) * 128, 2 * h + hh, :]

    def remote(src, dst, ssem, rsem, dev):
        return pltpu.make_async_remote_copy(
            src_ref=src, dst_ref=dst, send_sem=ssem, recv_sem=rsem,
            device_id=dev, device_id_type=MESH,
        )

    pl.semaphore_wait(barrier, len(peers))

    sends = []

    def start(copy):
        copy.start()
        sends.append(copy)

    def kv_own(j, h):
        lane = pl.multiple_of(h * 256, 256)
        return kvs.at[pl.ds(j * QUART, QUART), pl.ds(lane, 256)]

    def pos_own(j):
        return pos_ref.at[:, pl.ds(j * QUART, QUART)]

    for n in range(4):
        for d, zz in enumerate((z_up, z_down)):
            j = n // 2 if d == 0 else 1 - n // 2
            h = core if n % 2 == 0 else other
            slot = z * 4 + core * 2 + j
            start(remote(kv_own(j, h), kvb.at[slot], s_kv1.at[d, n], r_kv.at[slot], at(zz, xh, h)))
            start(remote(pos_own(j), posb.at[slot], s_pos1.at[d, n], r_pos.at[slot], at(zz, xh, h)))
    for h in range(2):
        dev = at(z, 1 - xh, h)
        start(remote(qs.at[h], qb.at[core], s_q.at[h], r_q.at[core], dev))
        start(remote(pos_ref, qpos.at[core], s_qp.at[h], r_qp.at[core], dev))
    for j in range(2):
        slot = z * 4 + core * 2 + j
        start(remote(kv_own(j, other), kvb.at[slot], s_loc.at[j], r_kv.at[slot], partner))
        start(remote(pos_own(j), posb.at[slot], s_locp.at[j], r_pos.at[slot], partner))
    start(remote(qs.at[other], qb.at[2 + core], s_q.at[2], r_q.at[2 + core], partner))
    start(remote(pos_ref, qpos.at[2 + core], s_qp.at[2], r_qp.at[2 + core], partner))

    qb[2 + core] = qs[core]
    qpos[2 + core] = pos_ref[...]
    mrun[...] = jnp.full(mrun.shape, NEG_BIG, F32)
    lrun[...] = jnp.zeros(lrun.shape, F32)
    acc[...] = jnp.zeros(acc.shape, F32)

    def place(step, at_quarter, kv, line):
        rows = pl.ds(pl.multiple_of(at_quarter * QUART, QUART), QUART)
        kb[step, rows, :] = kv[:, :HD]
        vtb[step, :, rows] = kv[:, HD:].T
        pkb[step, rows, :] = jnp.broadcast_to(line, (QUART, QUART)).T

    def wait_quarter(slot):
        remote(posb.at[slot], posb.at[slot], s_pos1.at[0, 0], r_pos.at[slot], partner).wait_recv()
        remote(kvb.at[slot], kvb.at[slot], s_kv1.at[0, 0], r_kv.at[slot], partner).wait_recv()

    own_lane = pl.multiple_of(core * 256, 256)
    for j in range(2):
        tokens = slice(j * QUART, (j + 1) * QUART)
        place(0, j, kvs[tokens, pl.ds(own_lane, 256)], pos_ref[:, tokens])
    for j in range(2):
        slot = z * 4 + other * 2 + j
        wait_quarter(slot)
        place(0, 2 + j, kvb[slot], posb[slot])

    w_copy.wait()

    def turn(i, carry):
        cols = pl.ds(pl.multiple_of(i * 128, 128), 128)
        wt[cols, :] = w_ref[:, cols].T
        return carry

    lax.fori_loop(0, 36, turn, 0)

    def service(i, carry):
        hop, a = i // 4 + 1, i % 4
        s = jnp.where(a % 2 == 0, core, other)
        for d in range(2):
            src_z = (z + NZ - hop) % NZ if d == 0 else (z + hop) % NZ
            j = a // 2 if d == 0 else 1 - a // 2
            slot = src_z * 4 + s * 2 + j
            dev = at(z_up if d == 0 else z_down, xh, core)
            wait_quarter(slot)

            @pl.when(i < 10)
            def _():
                remote(kvb.at[slot], kvb.at[slot], s_kvf.at[d, i], r_kv.at[slot], dev).start()
                remote(posb.at[slot], posb.at[slot], s_posf.at[d, i], r_pos.at[slot], dev).start()

            place(i // 2 + 1, (i % 2) * 2 + d, kvb[slot], posb[slot])
        return carry

    def attend(step):
        k = kb[step]
        vt = vtb[step]
        pk = pkb[step]
        blocks = [(g, half) for g in range(4) for half in range(2)]

        def scores(g, half):
            return lax.dot_general(k, qb[g, half], (((1,), (1,)), ((), ())), preferred_element_type=F32)

        s_next = scores(*blocks[0])
        for n, (g, half) in enumerate(blocks):
            s = s_next
            if n + 1 < len(blocks):
                s_next = scores(*blocks[n + 1])
            mask = pk <= qpos[g, :, half * 128:(half + 1) * 128]
            mask = jnp.concatenate([mask, mask], axis=1)
            s = jnp.where(mask, s * SCALE, NEG_BIG)
            cols = slice(half * 256, (half + 1) * 256)
            m_old = mrun[g, :, cols]
            m_new = jnp.maximum(m_old, jnp.max(s, axis=0, keepdims=True))
            p = jnp.exp2(s - m_new)
            alpha = jnp.exp2(m_old - m_new)
            part = jnp.sum(p.reshape(STEP_KEYS // 8, 8, 256), axis=0)
            lrun[g, :, cols] = lrun[g, :, cols] * alpha + part
            mrun[g, :, cols] = m_new
            add = jnp.dot(vt, p.astype(BF16), preferred_element_type=F32)
            acc[g, :, cols] = acc[g, :, cols] * alpha + add

    def round_of(j, done):
        until = jnp.where(j == 0, 4, jnp.where(j == 1, 5, jnp.where(j == 2, 7, jnp.where(j == 3, 8, jnp.where(j == 4, 9, 2 * j)))))
        lax.fori_loop(done, until, service, 0)

        @pl.when(j == 0)
        def _():
            for g in (2 + other, 0, 1):
                remote(qb.at[g], qb.at[g], s_q.at[0], r_q.at[g], partner).wait_recv()
                remote(qpos.at[g], qpos.at[g], s_qp.at[0], r_qp.at[g], partner).wait_recv()

        attend(j)
        return until

    lax.fori_loop(0, STEPS, round_of, 0)

    def finished(g):
        total = jnp.sum(lrun[g], axis=0, keepdims=True)
        lse = mrun[g] + jnp.log2(total)
        return (acc[g] * (1.0 / total)).astype(BF16), lse

    for g in range(2):
        o, lse = finished(g)
        stage[g] = o
        lstage[g] = lse
        dev = at(z, 1 - xh, g)
        start(remote(stage.at[g], attp.at[1, core], s_o.at[g], r_o.at[1, core], dev))
        start(remote(lstage.at[g], lsep.at[1, core], s_l.at[g], r_l.at[1, core], dev))
    o, lse = finished(2 + other)
    stage[2] = o
    lstage[2] = lse
    start(remote(stage.at[2], attp.at[0, core], s_o.at[2], r_o.at[0, core], partner))
    start(remote(lstage.at[2], lsep.at[0, core], s_l.at[2], r_l.at[0, core], partner))
    o, lse = finished(2 + core)
    attp[0, core] = o
    lsep[0, core] = lse

    def wait_part(p, h):
        remote(attp.at[p, h], attp.at[p, h], s_o.at[0], r_o.at[p, h], partner).wait_recv()
        remote(lsep.at[p, h], lsep.at[p, h], s_l.at[0], r_l.at[p, h], partner).wait_recv()

    wait_part(0, other)
    for h in range(2):
        wait_part(1, h)
        a, b = lsep[0, h], lsep[1, h]
        top = jnp.maximum(a, b)
        wa, wb = jnp.exp2(a - top), jnp.exp2(b - top)
        inv = 1.0 / (wa + wb)
        o = (attp[0, h].astype(F32) * (wa * inv) + attp[1, h].astype(F32) * (wb * inv)).astype(BF16)
        for half in range(2):
            for hh in range(2):
                lo = (2 * h + hh) * HD
                frm = half * 256 + hh * 128
                att[lo:lo + HD, half * 128:(half + 1) * 128] = o[:, frm:frm + 128]

    def terms(rel, b):
        row = ((y + rel) % 4) * (2 * OUT) + (xl if b == 0 else 1 - xl) * OUT
        rows = pl.ds(pl.multiple_of(row, 64), OUT)
        t = jnp.dot(wt[rows, :], att[...], preferred_element_type=F32)
        tt[rel * 2 + b] = t

    def chunk(k):
        return slice(k * YCHUNK, (k + 1) * YCHUNK), pl.ds(k * YCHUNK, YCHUNK)

    def send_y(kind, d, k):
        rows = chunk(k)[1]
        start(remote(ysend.at[kind, d, rows], yrecv.at[kind, d, rows], s_y.at[kind, d, k], r_y.at[kind, d, k], y_next[d]))

    def wait_y(kind, d, k):
        piece = yrecv.at[kind, d, chunk(k)[1]]
        remote(piece, piece, s_y.at[0, 0, 0], r_y.at[kind, d, k], x_pair).wait_recv()
        return yrecv[kind, d, chunk(k)[0], :].astype(F32)

    def send_x(rel):
        xsend[rel] = tt[rel * 2 + 1, YROWS:, :].astype(BF16)
        start(remote(xsend.at[rel], xrecv.at[rel], s_x.at[rel], r_x.at[rel], x_pair))

    def wait_x(rel):
        remote(xrecv.at[rel], xrecv.at[rel], s_x.at[0], r_x.at[rel], x_pair).wait_recv()
        tt[rel * 2, YROWS:, :] = tt[rel * 2, YROWS:, :] + xrecv[rel].astype(F32)

    def send_d(kind, d):
        start(remote(dsend.at[kind, d], drecv.at[kind, d], s_d.at[kind, d], r_d.at[kind, d], y_next[d]))

    def wait_d(kind, d):
        remote(drecv.at[kind, d], drecv.at[kind, d], s_d.at[0, 0], r_d.at[kind, d], x_pair).wait_recv()
        return drecv[kind, d].astype(F32)

    halves = (slice(YROWS, YROWS + XHALF), slice(YROWS + XHALF, OUT))

    terms(2, 1)
    ysend[0, 1] = tt[5, :YROWS, :].astype(BF16)
    send_y(0, 1, 0)
    send_y(0, 1, 1)
    send_x(2)
    terms(2, 0)
    ysend[0, 0] = tt[4, :YROWS, :].astype(BF16)
    send_y(0, 0, 0)
    send_y(0, 0, 1)
    terms(1, 1)
    ysend[1, 0] = tt[3, :YROWS, :].astype(BF16)
    send_y(1, 0, 0)
    send_y(1, 0, 1)
    send_x(1)
    terms(3, 0)
    ysend[1, 1] = tt[6, :YROWS, :].astype(BF16)
    send_y(1, 1, 0)
    send_y(1, 1, 1)
    terms(3, 1)
    send_x(3)
    terms(1, 0)
    terms(0, 1)
    send_x(0)
    terms(0, 0)
    wait_x(2)
    for d in range(2):
        dsend[0, d] = tt[4, halves[d], :].astype(BF16)
        send_d(0, d)
    for k in range(2):
        rows = chunk(k)[0]
        for d, n in ((0, 2), (1, 7)):
            got = wait_y(0, d, k)
            ysend[2, d, rows, :] = (tt[n, rows, :] + got).astype(BF16)
            send_y(2, d, k)
    for d, rel in ((0, 1), (1, 3)):
        wait_x(rel)
        dsend[1, d] = tt[2 * rel, halves[1 - d], :].astype(BF16)
        send_d(1, d)
    for d, rel in ((0, 1), (1, 3)):
        got = wait_d(0, d)
        dsend[2, d] = (tt[2 * rel, halves[d], :] + got).astype(BF16)
        send_d(2, d)
    wait_x(0)
    for k in range(2):
        rows = chunk(k)[0]
        full = tt[1, rows, :] + wait_y(1, 0, k) + wait_y(2, 1, k)
        psend[rows, :] = full.astype(BF16)
        start(remote(psend.at[chunk(k)[1]], precv.at[chunk(k)[1]], s_p.at[k], r_p.at[k], x_pair))
        tt[0, rows, :] = tt[0, rows, :] + wait_y(2, 0, k) + wait_y(1, 1, k)
    for d in range(2):
        full = tt[0, halves[d], :] + wait_d(2, d) + wait_d(1, 1 - d)
        out_ref[halves[d], :] = full.astype(BF16)
    for k in range(2):
        rows = chunk(k)[0]
        piece = precv.at[chunk(k)[1]]
        remote(piece, piece, s_p.at[0], r_p.at[k], x_pair).wait_recv()
        out_ref[rows, :] = (tt[0, rows, :] + precv[rows, :].astype(F32)).astype(BF16)

    for copy in sends:
        copy.wait_send()

    def drain(i, carry):
        for d in range(2):
            remote(kvb.at[0], kvb.at[0], s_kvf.at[d, i], r_kv.at[0], partner).wait_send()
            remote(posb.at[0], posb.at[0], s_posf.at[d, i], r_pos.at[0], partner).wait_send()
        return carry

    lax.fori_loop(0, 10, drain, 0)


def on_device(query_heads, key_heads, value_heads, positions, out_weight):
    pos = positions.reshape(1, TOK)
    dma = pltpu.SemaphoreType.DMA
    vmem = pl.BlockSpec(memory_space=pltpu.VMEM)
    out = pl.pallas_call(
        kernel,
        out_shape=jax.ShapeDtypeStruct((OUT, TOK), BF16),
        in_specs=[vmem, vmem, vmem, vmem, pl.BlockSpec(memory_space=pl.ANY)],
        out_specs=vmem,
        scratch_shapes=[
            pltpu.VMEM((TOK, 4 * HD), BF16),
            pltpu.VMEM((2, 2, 256, HD), BF16),
            pltpu.VMEM((4 * NZ, QUART, 2 * HD), BF16),
            pltpu.VMEM((4 * NZ, 1, QUART), jnp.int32),
            pltpu.VMEM((4, 2, 256, HD), BF16),
            pltpu.VMEM((4, 1, TOK), jnp.int32),
            pltpu.VMEM((STEPS, STEP_KEYS, HD), BF16),
            pltpu.VMEM((STEPS, HD, STEP_KEYS), BF16),
            pltpu.VMEM((STEPS, STEP_KEYS, QUART), jnp.int32),
            pltpu.VMEM((4, HD, LANES), F32),
            pltpu.VMEM((4, 1, LANES), F32),
            pltpu.VMEM((4, 8, LANES), F32),
            pltpu.VMEM((3, HD, LANES), BF16),
            pltpu.VMEM((3, 1, LANES), F32),
            pltpu.VMEM((2, 2, HD, LANES), BF16),
            pltpu.VMEM((2, 2, 1, LANES), F32),
            pltpu.VMEM((4 * HD, TOK), BF16),
            pltpu.VMEM((4 * HD, 8 * OUT), BF16),
            pltpu.VMEM((8 * OUT, 4 * HD), BF16),
            pltpu.VMEM((8, OUT, TOK), F32),
            pltpu.VMEM((3, 2, YROWS, TOK), BF16),
            pltpu.VMEM((3, 2, YROWS, TOK), BF16),
            pltpu.VMEM((4, XROWS, TOK), BF16),
            pltpu.VMEM((4, XROWS, TOK), BF16),
            pltpu.VMEM((3, 2, XHALF, TOK), BF16),
            pltpu.VMEM((3, 2, XHALF, TOK), BF16),
            pltpu.VMEM((YROWS, TOK), BF16),
            pltpu.VMEM((YROWS, TOK), BF16),
            dma((2, 4)), dma((2, 10)), dma((2, 4)), dma((2, 10)), dma((2,)), dma((2,)),
            dma((3,)), dma((3,)), dma((3,)), dma((3,)),
            dma((3, 2, 2)), dma((4,)), dma((3, 2)), dma((2,)),
            dma((4 * NZ,)), dma((4 * NZ,)), dma((4,)), dma((4,)), dma((2, 2)), dma((2, 2)),
            dma((3, 2, 2)), dma((4,)), dma((3, 2)), dma((2,)), dma,
        ],
        compiler_params=pltpu.CompilerParams(
            collective_id=0, has_side_effects=True, vmem_limit_bytes=60 * 1024 * 1024
        ),
        cost_estimate=pl.CostEstimate(flops=6_000_000_000, bytes_accessed=6_000_000, transcendentals=8_000_000),
    )(query_heads, key_heads, value_heads, pos, out_weight)
    return out.T


def solution(mesh):
    return jax.shard_map(
        on_device,
        mesh=mesh,
        in_specs=(
            P("ctx", "head", None),
            P("ctx", "head", None),
            P("ctx", "head", None),
            P("ctx"),
            P("head", None),
        ),
        out_specs=P("ctx", "head"),
        check_vma=False,
    )
```

```python
import jax
import jax.numpy as jnp
from jax import lax
from jax.experimental import pallas as pl
from jax.experimental.pallas import tpu as pltpu
from jax.sharding import PartitionSpec as P

MESH = pl.DeviceIdType.MESH
NEG_BIG = -1e30
LOG2E = 1.4426950408889634
SCALE = LOG2E / 12.0
NZ = 8
TOK = 256
QUART = 128
HD = 128
STEPS = NZ
STEP_KEYS = 512
HALF = 256
OUT = 576
YROWS = 352
XROWS = OUT - YROWS
XHALF = XROWS // 2
F32 = jnp.float32
BF16 = jnp.bfloat16


def kernel(
    q_hbm, k_hbm, v_hbm, pos_hbm, w_hbm, out_ref,
    q_ref, k_ref, v_ref, pos_ref, wide, kvs, qs, kvb, posb, qb, qpos, kb, vtb, pkb, acc, mrun, lrun,
    stage, lstage, attp, lsep, att, w_ref, wt,
    tt, ysend, yrecv, xsend, xrecv, dsend, drecv, psend, precv,
    s_kv1, s_kvf, s_pos1, s_posf, s_loc, s_locp, s_q, s_qp, s_o, s_l,
    s_y, s_x, s_d, s_p,
    r_kv, r_pos, r_q, r_qp, r_o, r_l, r_y, r_x, r_d, r_p, in_sem,
):
    ctx, head = lax.axis_index("ctx"), lax.axis_index("head")
    core, xh, z = ctx % 2, (ctx // 2) % 2, ctx // 4
    y, xl = head // 2, head % 2
    other = 1 - core

    def at(zz, xx, cc):
        return ((zz * 2 + xx) * 2 + cc, head)

    z_up, z_down = (z + 1) % NZ, (z + NZ - 1) % NZ
    partner = at(z, xh, other)
    y_next = ((ctx, ((y + 1) % 4) * 2 + xl), (ctx, ((y + 3) % 4) * 2 + xl))
    x_pair = (ctx, y * 2 + 1 - xl)
    peers = [partner, y_next[0], y_next[1], x_pair]
    for cc in range(2):
        peers += [at(z_up, xh, cc), at(z_down, xh, cc), at(z, 1 - xh, cc)]
    barrier = pltpu.get_barrier_semaphore()
    for peer in peers:
        pl.semaphore_signal(barrier, inc=1, device_id=peer, device_id_type=MESH)

    loads = []
    for n, (src, dst) in enumerate(((k_hbm, k_ref), (v_hbm, v_ref), (pos_hbm, pos_ref), (q_hbm, q_ref), (w_hbm, w_ref))):
        loads.append(pltpu.make_async_copy(src, dst, in_sem.at[n]))
        loads[n].start()

    for n, ref in enumerate((k_ref, v_ref)):
        loads[n].wait()
        wide[n * 512:(n + 1) * 512, :] = ref[...].astype(F32)
        for h in range(2):
            lo = h * 256 + n * HD
            kvs[:, lo:lo + HD] = wide[pl.ds(n * 512 + h, TOK, stride=2), :].astype(BF16)
    loads[2].wait()

    def remote(src, dst, ssem, rsem, dev):
        return pltpu.make_async_remote_copy(
            src_ref=src, dst_ref=dst, send_sem=ssem, recv_sem=rsem,
            device_id=dev, device_id_type=MESH,
        )

    pl.semaphore_wait(barrier, len(peers))

    sends = []

    def start(copy):
        copy.start()
        sends.append(copy)

    def kv_own(j, h):
        lane = pl.multiple_of(h * 256, 256)
        return kvs.at[pl.ds(j * QUART, QUART), pl.ds(lane, 256)]

    def pos_own(j):
        return pos_ref.at[:, pl.ds(j * QUART, QUART)]

    for n in range(4):
        for d, zz in enumerate((z_up, z_down)):
            j = n // 2 if d == 0 else 1 - n // 2
            h = core if n % 2 == 0 else other
            slot = z * 4 + core * 2 + j
            start(remote(kv_own(j, h), kvb.at[slot], s_kv1.at[d, n], r_kv.at[slot], at(zz, xh, h)))
            start(remote(pos_own(j), posb.at[slot], s_pos1.at[d, n], r_pos.at[slot], at(zz, xh, h)))
    for j in range(2):
        slot = z * 4 + core * 2 + j
        start(remote(kv_own(j, other), kvb.at[slot], s_loc.at[j], r_kv.at[slot], partner))
        start(remote(pos_own(j), posb.at[slot], s_locp.at[j], r_pos.at[slot], partner))

    loads[3].wait()
    wide[...] = q_ref[...].astype(F32)
    for h in range(2):
        for half in range(2):
            for hh in range(2):
                rows = pl.ds(half * 512 + 2 * h + hh, 128, stride=4)
                qs[h, half, hh * 128:(hh + 1) * 128, :] = wide[rows, :].astype(BF16)
    start(remote(qs.at[other], qb.at[2 + core], s_q.at[2], r_q.at[2 + core], partner))
    start(remote(pos_ref, qpos.at[2 + core], s_qp.at[2], r_qp.at[2 + core], partner))
    for h in range(2):
        dev = at(z, 1 - xh, h)
        start(remote(qs.at[h], qb.at[core], s_q.at[h], r_q.at[core], dev))
        start(remote(pos_ref, qpos.at[core], s_qp.at[h], r_qp.at[core], dev))

    qb[2 + core] = qs[core]
    qpos[2 + core] = pos_ref[...]
    mrun[...] = jnp.full(mrun.shape, NEG_BIG, F32)
    lrun[...] = jnp.zeros(lrun.shape, F32)
    acc[...] = jnp.zeros(acc.shape, F32)

    def place(step, at_quarter, kv, line):
        rows = pl.ds(pl.multiple_of(at_quarter * QUART, QUART), QUART)
        kb[step, rows, :] = kv[:, :HD]
        vtb[step, :, rows] = kv[:, HD:].T
        pkb[step, rows, :] = jnp.broadcast_to(line, (QUART, QUART)).T

    def wait_quarter(slot):
        remote(posb.at[slot], posb.at[slot], s_pos1.at[0, 0], r_pos.at[slot], partner).wait_recv()
        remote(kvb.at[slot], kvb.at[slot], s_kv1.at[0, 0], r_kv.at[slot], partner).wait_recv()

    own_lane = pl.multiple_of(core * 256, 256)
    for j in range(2):
        tokens = slice(j * QUART, (j + 1) * QUART)
        place(0, j, kvs[tokens, pl.ds(own_lane, 256)], pos_ref[:, tokens])
    def turn(i, carry):
        cols = pl.ds(pl.multiple_of(i * 128, 128), 128)
        wt[cols, :] = w_ref[:, cols].T
        return carry

    loads[4].wait()
    lax.fori_loop(0, 36, turn, 0)

    for j in range(2):
        slot = z * 4 + other * 2 + j
        wait_quarter(slot)
        place(0, 2 + j, kvb[slot], posb[slot])

    def wait_queries(g):
        remote(qb.at[g], qb.at[g], s_q.at[0], r_q.at[g], partner).wait_recv()
        remote(qpos.at[g], qpos.at[g], s_qp.at[0], r_qp.at[g], partner).wait_recv()

    wait_queries(2 + other)

    def service(i, carry):
        hop, a = i // 4 + 1, i % 4
        s = jnp.where(a % 2 == 0, core, other)
        for d in range(2):
            src_z = (z + NZ - hop) % NZ if d == 0 else (z + hop) % NZ
            j = a // 2 if d == 0 else 1 - a // 2
            slot = src_z * 4 + s * 2 + j
            dev = at(z_up if d == 0 else z_down, xh, core)
            wait_quarter(slot)

            @pl.when(i < 10)
            def _():
                remote(kvb.at[slot], kvb.at[slot], s_kvf.at[d, i], r_kv.at[slot], dev).start()
                remote(posb.at[slot], posb.at[slot], s_posf.at[d, i], r_pos.at[slot], dev).start()

            place(i // 2 + 1, (i % 2) * 2 + d, kvb[slot], posb[slot])
        return carry

    def attend(step, first):
        k = kb[step]
        vt = vtb[step]
        pk = pkb[step]
        blocks = [(first + n, half) for n in range(2) for half in range(2)]

        def scores(g, half):
            return lax.dot_general(k, qb[g, half], (((1,), (1,)), ((), ())), preferred_element_type=F32)

        s_next = scores(*blocks[0])
        for n, (g, half) in enumerate(blocks):
            s = s_next
            if n + 1 < len(blocks):
                s_next = scores(*blocks[n + 1])
            mask = pk <= qpos[g, :, half * 128:(half + 1) * 128]
            mask = jnp.concatenate([mask, mask], axis=1)
            s = jnp.where(mask, s, NEG_BIG)
            m_old = mrun[g, half]
            m_new = jnp.maximum(m_old, jnp.max(s, axis=0, keepdims=True))
            p = jnp.exp2((s - m_new) * SCALE)
            alpha = jnp.exp2((m_old - m_new) * SCALE)
            part = jnp.sum(p.reshape(STEP_KEYS // 8, 8, HALF), axis=0)
            lrun[g, half] = lrun[g, half] * alpha + part
            mrun[g, half] = m_new
            add = jnp.dot(vt, p.astype(BF16), preferred_element_type=F32)
            acc[g, half] = acc[g, half] * alpha + add

    plan = (
        (0, 0, 2), (2, 1, 2), (4, 2, 2), (4, 0, 0), (5, 1, 0), (6, 3, 2), (6, 2, 0), (7, 3, 0),
        (8, 4, 2), (8, 4, 0), (10, 5, 2), (10, 5, 0), (12, 6, 2), (12, 6, 0), (14, 7, 0),
    )

    def planned(n, column):
        value = plan[0][column]
        for m in range(1, len(plan)):
            value = jnp.where(n == m, plan[m][column], value)
        return value

    def round_of(n, done):
        until = planned(n, 0)
        lax.fori_loop(done, until, service, 0)

        @pl.when(n == 3)
        def _():
            for g in range(2):
                wait_queries(g)

        attend(planned(n, 1), planned(n, 2))
        return until

    lax.fori_loop(0, len(plan), round_of, 0)

    def finished(g, half):
        total = jnp.sum(lrun[g, half], axis=0, keepdims=True)
        lse = mrun[g, half] * SCALE + jnp.log2(total)
        return (acc[g, half] * (1.0 / total)).astype(BF16), lse

    def give_back(n, g, half, p, dev):
        o, lse = finished(g, half)
        stage[n, half] = o
        lstage[n, half] = lse
        start(remote(stage.at[n, half], attp.at[p, core, half], s_o.at[n, half], r_o.at[p, core, half], dev))
        start(remote(lstage.at[n, half], lsep.at[p, core, half], s_l.at[n, half], r_l.at[p, core, half], dev))

    for half in range(2):
        for g in range(2):
            give_back(g, g, half, 1, at(z, 1 - xh, g))
    attend(STEPS - 1, 2)
    for half in range(2):
        give_back(2, 2 + other, half, 0, partner)
    for half in range(2):
        o, lse = finished(2 + core, half)
        attp[0, core, half] = o
        lsep[0, core, half] = lse

    def wait_part(p, h, half):
        o, lse = attp.at[p, h, half], lsep.at[p, h, half]
        remote(o, o, s_o.at[0, 0], r_o.at[p, h, half], partner).wait_recv()
        remote(lse, lse, s_l.at[0, 0], r_l.at[p, h, half], partner).wait_recv()

    def merge(half):
        wait_part(0, other, half)
        for h in range(2):
            wait_part(1, h, half)
            a, b = lsep[0, h, half], lsep[1, h, half]
            top = jnp.maximum(a, b)
            wa, wb = jnp.exp2(a - top), jnp.exp2(b - top)
            inv = 1.0 / (wa + wb)
            o = (attp[0, h, half].astype(F32) * (wa * inv) + attp[1, h, half].astype(F32) * (wb * inv)).astype(BF16)
            for hh in range(2):
                lo = (2 * h + hh) * HD
                att[half, lo:lo + HD, :] = o[:, hh * 128:(hh + 1) * 128]

    def terms(wave, rel, b):
        row = ((y + rel) % 4) * (2 * OUT) + (xl if b == 0 else 1 - xl) * OUT
        rows = pl.ds(pl.multiple_of(row, 64), OUT)
        tt[wave, rel * 2 + b] = jnp.dot(wt[rows, :], att[wave], preferred_element_type=F32)

    def send_y(wave, kind, d):
        start(remote(ysend.at[wave, kind, d], yrecv.at[wave, kind, d], s_y.at[wave, kind, d], r_y.at[wave, kind, d], y_next[d]))

    def wait_y(wave, kind, d):
        piece = yrecv.at[wave, kind, d]
        remote(piece, piece, s_y.at[0, 0, 0], r_y.at[wave, kind, d], x_pair).wait_recv()
        return yrecv[wave, kind, d].astype(F32)

    def first_y(wave, kind, d, rel, b):
        ysend[wave, kind, d] = tt[wave, rel * 2 + b, :YROWS, :].astype(BF16)
        send_y(wave, kind, d)

    def send_x(wave, rel):
        xsend[wave, rel] = tt[wave, rel * 2 + 1, YROWS:, :].astype(BF16)
        start(remote(xsend.at[wave, rel], xrecv.at[wave, rel], s_x.at[wave, rel], r_x.at[wave, rel], x_pair))

    def wait_x(wave, rel):
        piece = xrecv.at[wave, rel]
        remote(piece, piece, s_x.at[0, 0], r_x.at[wave, rel], x_pair).wait_recv()
        tt[wave, rel * 2, YROWS:, :] = tt[wave, rel * 2, YROWS:, :] + xrecv[wave, rel].astype(F32)

    def send_d(wave, kind, d):
        start(remote(dsend.at[wave, kind, d], drecv.at[wave, kind, d], s_d.at[wave, kind, d], r_d.at[wave, kind, d], y_next[d]))

    def wait_d(wave, kind, d):
        piece = drecv.at[wave, kind, d]
        remote(piece, piece, s_d.at[0, 0, 0], r_d.at[wave, kind, d], x_pair).wait_recv()
        return drecv[wave, kind, d].astype(F32)

    halves = (slice(YROWS, YROWS + XHALF), slice(YROWS + XHALF, OUT))

    for w in range(2):
        merge(w)
        terms(w, 2, 1)
        first_y(w, 0, 1, 2, 1)
        send_x(w, 2)
        terms(w, 2, 0)
        first_y(w, 0, 0, 2, 0)
        terms(w, 1, 1)
        first_y(w, 1, 0, 1, 1)
        send_x(w, 1)
        terms(w, 3, 0)
        first_y(w, 1, 1, 3, 0)
        terms(w, 3, 1)
        send_x(w, 3)
        terms(w, 1, 0)
        terms(w, 0, 1)
        send_x(w, 0)
        terms(w, 0, 0)
    for w in range(2):
        for d, n in ((0, 2), (1, 7)):
            got = wait_y(w, 0, d)
            ysend[w, 2, d] = (tt[w, n, :YROWS, :] + got).astype(BF16)
            send_y(w, 2, d)
        wait_x(w, 2)
        for d in range(2):
            dsend[w, 0, d] = tt[w, 4, halves[d], :].astype(BF16)
            send_d(w, 0, d)
        for d, rel in ((0, 1), (1, 3)):
            wait_x(w, rel)
            dsend[w, 1, d] = tt[w, 2 * rel, halves[1 - d], :].astype(BF16)
            send_d(w, 1, d)
    for w in range(2):
        for d, rel in ((0, 1), (1, 3)):
            got = wait_d(w, 0, d)
            dsend[w, 2, d] = (tt[w, 2 * rel, halves[d], :] + got).astype(BF16)
            send_d(w, 2, d)
        full = tt[w, 1, :YROWS, :] + wait_y(w, 1, 0) + wait_y(w, 2, 1)
        psend[w] = full.astype(BF16)
        start(remote(psend.at[w], precv.at[w], s_p.at[w], r_p.at[w], x_pair))
        tt[w, 0, :YROWS, :] = tt[w, 0, :YROWS, :] + wait_y(w, 2, 0) + wait_y(w, 1, 1)
    for w in range(2):
        lanes = slice(w * 128, (w + 1) * 128)
        wait_x(w, 0)
        for d in range(2):
            out_ref[halves[d], lanes] = tt[w, 0, halves[d], :] + wait_d(w, 2, d) + wait_d(w, 1, 1 - d)
        remote(precv.at[w], precv.at[w], s_p.at[0], r_p.at[w], x_pair).wait_recv()
        out_ref[:YROWS, lanes] = tt[w, 0, :YROWS, :] + precv[w].astype(F32)

    for copy in sends:
        copy.wait_send()

    def drain(i, carry):
        for d in range(2):
            remote(kvb.at[0], kvb.at[0], s_kvf.at[d, i], r_kv.at[0], partner).wait_send()
            remote(posb.at[0], posb.at[0], s_posf.at[d, i], r_pos.at[0], partner).wait_send()
        return carry

    lax.fori_loop(0, 10, drain, 0)


def on_device(query_heads, key_heads, value_heads, positions, out_weight):
    dma = pltpu.SemaphoreType.DMA
    hbm = pl.BlockSpec(memory_space=pl.ANY)
    out = pl.pallas_call(
        kernel,
        out_shape=jax.ShapeDtypeStruct((OUT, TOK), F32),
        in_specs=[hbm] * 5,
        out_specs=pl.BlockSpec(memory_space=pltpu.VMEM),
        scratch_shapes=[
            pltpu.VMEM((4 * TOK, HD), BF16),
            pltpu.VMEM((2 * TOK, HD), BF16),
            pltpu.VMEM((2 * TOK, HD), BF16),
            pltpu.VMEM((1, TOK), jnp.int32),
            pltpu.VMEM((4 * TOK, HD), F32),
            pltpu.VMEM((TOK, 4 * HD), BF16),
            pltpu.VMEM((2, 2, 256, HD), BF16),
            pltpu.VMEM((4 * NZ, QUART, 2 * HD), BF16),
            pltpu.VMEM((4 * NZ, 1, QUART), jnp.int32),
            pltpu.VMEM((4, 2, 256, HD), BF16),
            pltpu.VMEM((4, 1, TOK), jnp.int32),
            pltpu.VMEM((STEPS, STEP_KEYS, HD), BF16),
            pltpu.VMEM((STEPS, HD, STEP_KEYS), BF16),
            pltpu.VMEM((STEPS, STEP_KEYS, QUART), jnp.int32),
            pltpu.VMEM((4, 2, HD, HALF), F32),
            pltpu.VMEM((4, 2, 1, HALF), F32),
            pltpu.VMEM((4, 2, 8, HALF), F32),
            pltpu.VMEM((3, 2, HD, HALF), BF16),
            pltpu.VMEM((3, 2, 1, HALF), F32),
            pltpu.VMEM((2, 2, 2, HD, HALF), BF16),
            pltpu.VMEM((2, 2, 2, 1, HALF), F32),
            pltpu.VMEM((2, 4 * HD, 128), BF16),
            pltpu.VMEM((4 * HD, 8 * OUT), BF16),
            pltpu.VMEM((8 * OUT, 4 * HD), BF16),
            pltpu.VMEM((2, 8, OUT, 128), F32),
            pltpu.VMEM((2, 3, 2, YROWS, 128), BF16),
            pltpu.VMEM((2, 3, 2, YROWS, 128), BF16),
            pltpu.VMEM((2, 4, XROWS, 128), BF16),
            pltpu.VMEM((2, 4, XROWS, 128), BF16),
            pltpu.VMEM((2, 3, 2, XHALF, 128), BF16),
            pltpu.VMEM((2, 3, 2, XHALF, 128), BF16),
            pltpu.VMEM((2, YROWS, 128), BF16),
            pltpu.VMEM((2, YROWS, 128), BF16),
            dma((2, 4)), dma((2, 10)), dma((2, 4)), dma((2, 10)), dma((2,)), dma((2,)),
            dma((3,)), dma((3,)), dma((3, 2)), dma((3, 2)),
            dma((2, 3, 2)), dma((2, 4)), dma((2, 3, 2)), dma((2,)),
            dma((4 * NZ,)), dma((4 * NZ,)), dma((4,)), dma((4,)), dma((2, 2, 2)), dma((2, 2, 2)),
            dma((2, 3, 2)), dma((2, 4)), dma((2, 3, 2)), dma((2,)), dma((5,)),
        ],
        compiler_params=pltpu.CompilerParams(
            collective_id=0, has_side_effects=True, vmem_limit_bytes=60 * 1024 * 1024
        ),
        cost_estimate=pl.CostEstimate(flops=6_000_000_000, bytes_accessed=6_000_000, transcendentals=8_000_000),
    )(
        query_heads.reshape(4 * TOK, HD), key_heads.reshape(2 * TOK, HD), value_heads.reshape(2 * TOK, HD),
        positions.reshape(1, TOK), out_weight,
    )
    return out.astype(BF16).T


def solution(mesh):
    return jax.shard_map(
        on_device,
        mesh=mesh,
        in_specs=(
            P("ctx", "head", None),
            P("ctx", "head", None),
            P("ctx", "head", None),
            P("ctx"),
            P("head", None),
        ),
        out_specs=P("ctx", "head"),
        check_vma=False,
    )
```

```python
import jax
import jax.numpy as jnp
from jax import lax
from jax.experimental import pallas as pl
from jax.experimental.pallas import tpu as pltpu
from jax.sharding import PartitionSpec as P

MESH = pl.DeviceIdType.MESH
NEG_BIG = -1e30
LOG2E = 1.4426950408889634
SCALE = LOG2E / 12.0
NZ = 8
TOK = 256
QUART = 128
HD = 128
STEPS = NZ
STEP_KEYS = 512
HALF = 256
OUT = 576
YROWS = 288
XROWS = OUT - YROWS
XHALF = XROWS // 2
F32 = jnp.float32
BF16 = jnp.bfloat16


def kernel(
    q_hbm, k_hbm, v_hbm, pos_hbm, w_hbm, out_ref,
    q_ref, k_ref, v_ref, pos_ref, wide, kvs, qs, kvb, posb, qb, qpos, kb, vtb, pkb, acc, mrun, lrun,
    stage, lstage, attp, lsep, att, w_ref, wt,
    tt, ysend, yrecv, xsend, xrecv, dsend, drecv, psend, precv,
    s_kv1, s_kvf, s_pos1, s_posf, s_loc, s_locp, s_q, s_qp, s_o, s_l,
    s_y, s_x, s_d, s_p,
    r_kv, r_pos, r_q, r_qp, r_o, r_l, r_y, r_x, r_d, r_p, in_sem,
):
    ctx, head = lax.axis_index("ctx"), lax.axis_index("head")
    core, xh, z = ctx % 2, (ctx // 2) % 2, ctx // 4
    y, xl = head // 2, head % 2
    other = 1 - core

    def at(zz, xx, cc):
        return ((zz * 2 + xx) * 2 + cc, head)

    z_up, z_down = (z + 1) % NZ, (z + NZ - 1) % NZ
    partner = at(z, xh, other)
    y_next = ((ctx, ((y + 1) % 4) * 2 + xl), (ctx, ((y + 3) % 4) * 2 + xl))
    x_pair = (ctx, y * 2 + 1 - xl)
    peers = [partner, y_next[0], y_next[1], x_pair]
    for cc in range(2):
        peers += [at(z_up, xh, cc), at(z_down, xh, cc), at(z, 1 - xh, cc)]
    barrier = pltpu.get_barrier_semaphore()
    for peer in peers:
        pl.semaphore_signal(barrier, inc=1, device_id=peer, device_id_type=MESH)

    loads = []
    for n, (src, dst) in enumerate(((k_hbm, k_ref), (v_hbm, v_ref), (pos_hbm, pos_ref), (q_hbm, q_ref), (w_hbm, w_ref))):
        loads.append(pltpu.make_async_copy(src, dst, in_sem.at[n]))
        loads[n].start()

    for n, ref in enumerate((k_ref, v_ref)):
        loads[n].wait()
        wide[n * 512:(n + 1) * 512, :] = ref[...].astype(F32)
        for h in range(2):
            lo = h * 256 + n * HD
            kvs[:, lo:lo + HD] = wide[pl.ds(n * 512 + h, TOK, stride=2), :].astype(BF16)
    loads[2].wait()

    def remote(src, dst, ssem, rsem, dev):
        return pltpu.make_async_remote_copy(
            src_ref=src, dst_ref=dst, send_sem=ssem, recv_sem=rsem,
            device_id=dev, device_id_type=MESH,
        )

    pl.semaphore_wait(barrier, len(peers))

    sends = []

    def start(copy):
        copy.start()
        sends.append(copy)

    def kv_own(j, h):
        lane = pl.multiple_of(h * 256, 256)
        return kvs.at[pl.ds(j * QUART, QUART), pl.ds(lane, 256)]

    def pos_own(j):
        return pos_ref.at[:, pl.ds(j * QUART, QUART)]

    for n in range(4):
        for d, zz in enumerate((z_up, z_down)):
            j = n // 2 if d == 0 else 1 - n // 2
            h = core if n % 2 == 0 else other
            slot = z * 4 + core * 2 + j
            start(remote(kv_own(j, h), kvb.at[slot], s_kv1.at[d, n], r_kv.at[slot], at(zz, xh, h)))
            start(remote(pos_own(j), posb.at[slot], s_pos1.at[d, n], r_pos.at[slot], at(zz, xh, h)))
    for j in range(2):
        slot = z * 4 + core * 2 + j
        start(remote(kv_own(j, other), kvb.at[slot], s_loc.at[j], r_kv.at[slot], partner))
        start(remote(pos_own(j), posb.at[slot], s_locp.at[j], r_pos.at[slot], partner))

    loads[3].wait()
    wide[...] = q_ref[...].astype(F32)
    for h in range(2):
        for half in range(2):
            for hh in range(2):
                rows = pl.ds(half * 512 + 2 * h + hh, 128, stride=4)
                qs[h, half, hh * 128:(hh + 1) * 128, :] = wide[rows, :].astype(BF16)
    start(remote(qs.at[other], qb.at[2 + core], s_q.at[2], r_q.at[2 + core], partner))
    start(remote(pos_ref, qpos.at[2 + core], s_qp.at[2], r_qp.at[2 + core], partner))
    for h in range(2):
        dev = at(z, 1 - xh, h)
        start(remote(qs.at[h], qb.at[core], s_q.at[h], r_q.at[core], dev))
        start(remote(pos_ref, qpos.at[core], s_qp.at[h], r_qp.at[core], dev))

    qb[2 + core] = qs[core]
    qpos[2 + core] = pos_ref[...]
    mrun[...] = jnp.full(mrun.shape, NEG_BIG, F32)
    lrun[...] = jnp.zeros(lrun.shape, F32)
    acc[...] = jnp.zeros(acc.shape, F32)

    def place(step, at_quarter, kv, line):
        rows = pl.ds(pl.multiple_of(at_quarter * QUART, QUART), QUART)
        kb[step, rows, :] = kv[:, :HD]
        vtb[step, :, rows] = kv[:, HD:].T
        pkb[step, rows, :] = jnp.broadcast_to(line, (QUART, QUART)).T

    def wait_quarter(slot):
        remote(posb.at[slot], posb.at[slot], s_pos1.at[0, 0], r_pos.at[slot], partner).wait_recv()
        remote(kvb.at[slot], kvb.at[slot], s_kv1.at[0, 0], r_kv.at[slot], partner).wait_recv()

    own_lane = pl.multiple_of(core * 256, 256)
    for j in range(2):
        tokens = slice(j * QUART, (j + 1) * QUART)
        place(0, j, kvs[tokens, pl.ds(own_lane, 256)], pos_ref[:, tokens])
    def turn(i, carry):
        cols = pl.ds(pl.multiple_of(i * 128, 128), 128)
        wt[cols, :] = w_ref[:, cols].T
        return carry

    loads[4].wait()
    lax.fori_loop(0, 36, turn, 0)

    for j in range(2):
        slot = z * 4 + other * 2 + j
        wait_quarter(slot)
        place(0, 2 + j, kvb[slot], posb[slot])

    def wait_queries(g):
        remote(qb.at[g], qb.at[g], s_q.at[0], r_q.at[g], partner).wait_recv()
        remote(qpos.at[g], qpos.at[g], s_qp.at[0], r_qp.at[g], partner).wait_recv()

    wait_queries(2 + other)

    def service(i, carry):
        hop, a = i // 4 + 1, i % 4
        s = jnp.where(a % 2 == 0, core, other)
        for d in range(2):
            src_z = (z + NZ - hop) % NZ if d == 0 else (z + hop) % NZ
            j = a // 2 if d == 0 else 1 - a // 2
            slot = src_z * 4 + s * 2 + j
            dev = at(z_up if d == 0 else z_down, xh, core)
            wait_quarter(slot)

            @pl.when(i < 10)
            def _():
                remote(kvb.at[slot], kvb.at[slot], s_kvf.at[d, i], r_kv.at[slot], dev).start()
                remote(posb.at[slot], posb.at[slot], s_posf.at[d, i], r_pos.at[slot], dev).start()

            place(i // 2 + 1, (i % 2) * 2 + d, kvb[slot], posb[slot])
        return carry

    def attend(step, first):
        k = kb[step]
        vt = vtb[step]
        pk = pkb[step]
        blocks = [(first + n, half) for n in range(2) for half in range(2)]

        def scores(g, half):
            return lax.dot_general(k, qb[g, half], (((1,), (1,)), ((), ())), preferred_element_type=F32)

        s_next = scores(*blocks[0])
        for n, (g, half) in enumerate(blocks):
            s = s_next
            if n + 1 < len(blocks):
                s_next = scores(*blocks[n + 1])
            mask = pk <= qpos[g, :, half * 128:(half + 1) * 128]
            mask = jnp.concatenate([mask, mask], axis=1)
            s = jnp.where(mask, s, NEG_BIG)
            m_old = mrun[g, half]
            m_new = jnp.maximum(m_old, jnp.max(s, axis=0, keepdims=True))
            p = jnp.exp2((s - m_new) * SCALE)
            alpha = jnp.exp2((m_old - m_new) * SCALE)
            part = jnp.sum(p.reshape(STEP_KEYS // 8, 8, HALF), axis=0)
            lrun[g, half] = lrun[g, half] * alpha + part
            mrun[g, half] = m_new
            add = jnp.dot(vt, p.astype(BF16), preferred_element_type=F32)
            acc[g, half] = acc[g, half] * alpha + add

    plan = (
        (0, 0, 2), (2, 1, 2), (4, 2, 2), (4, 0, 0), (5, 1, 0), (6, 3, 2), (6, 2, 0), (7, 3, 0),
        (8, 4, 2), (8, 4, 0), (10, 5, 2), (10, 5, 0), (12, 6, 2), (12, 6, 0), (14, 7, 0),
    )

    def planned(n, column):
        value = plan[0][column]
        for m in range(1, len(plan)):
            value = jnp.where(n == m, plan[m][column], value)
        return value

    def round_of(n, done):
        until = planned(n, 0)
        lax.fori_loop(done, until, service, 0)

        @pl.when(n == 3)
        def _():
            for g in range(2):
                wait_queries(g)

        attend(planned(n, 1), planned(n, 2))
        return until

    lax.fori_loop(0, len(plan), round_of, 0)

    def finished(g, half):
        total = jnp.sum(lrun[g, half], axis=0, keepdims=True)
        lse = mrun[g, half] * SCALE + jnp.log2(total)
        return (acc[g, half] * (1.0 / total)).astype(BF16), lse

    def give_back(n, g, half, p, dev):
        o, lse = finished(g, half)
        stage[n, half] = o
        lstage[n, half] = lse
        start(remote(stage.at[n, half], attp.at[p, core, half], s_o.at[n, half], r_o.at[p, core, half], dev))
        start(remote(lstage.at[n, half], lsep.at[p, core, half], s_l.at[n, half], r_l.at[p, core, half], dev))

    for half in range(2):
        for g in range(2):
            give_back(g, g, half, 1, at(z, 1 - xh, g))
    attend(STEPS - 1, 2)
    for half in range(2):
        give_back(2, 2 + other, half, 0, partner)
    for half in range(2):
        o, lse = finished(2 + core, half)
        attp[0, core, half] = o
        lsep[0, core, half] = lse

    def wait_part(p, h, half):
        o, lse = attp.at[p, h, half], lsep.at[p, h, half]
        remote(o, o, s_o.at[0, 0], r_o.at[p, h, half], partner).wait_recv()
        remote(lse, lse, s_l.at[0, 0], r_l.at[p, h, half], partner).wait_recv()

    def merge(half):
        wait_part(0, other, half)
        for h in range(2):
            wait_part(1, h, half)
            a, b = lsep[0, h, half], lsep[1, h, half]
            top = jnp.maximum(a, b)
            wa, wb = jnp.exp2(a - top), jnp.exp2(b - top)
            inv = 1.0 / (wa + wb)
            o = (attp[0, h, half].astype(F32) * (wa * inv) + attp[1, h, half].astype(F32) * (wb * inv)).astype(BF16)
            for hh in range(2):
                lo = (2 * h + hh) * HD
                att[half, lo:lo + HD, :] = o[:, hh * 128:(hh + 1) * 128]

    def terms(wave, rel, b):
        row = ((y + rel) % 4) * (2 * OUT) + (xl if b == 0 else 1 - xl) * OUT
        rows = pl.ds(pl.multiple_of(row, 64), OUT)
        tt[wave, rel * 2 + b] = jnp.dot(wt[rows, :], att[wave], preferred_element_type=F32)

    def send_y(wave, kind, d):
        start(remote(ysend.at[wave, kind, d], yrecv.at[wave, kind, d], s_y.at[wave, kind, d], r_y.at[wave, kind, d], y_next[d]))

    def wait_y(wave, kind, d):
        piece = yrecv.at[wave, kind, d]
        remote(piece, piece, s_y.at[0, 0, 0], r_y.at[wave, kind, d], x_pair).wait_recv()
        return yrecv[wave, kind, d].astype(F32)

    def first_y(wave, kind, d, rel, b):
        ysend[wave, kind, d] = tt[wave, rel * 2 + b, :YROWS, :].astype(BF16)
        send_y(wave, kind, d)

    def send_x(wave, rel):
        xsend[wave, rel] = tt[wave, rel * 2 + 1, YROWS:, :].astype(BF16)
        start(remote(xsend.at[wave, rel], xrecv.at[wave, rel], s_x.at[wave, rel], r_x.at[wave, rel], x_pair))

    def wait_x(wave, rel):
        piece = xrecv.at[wave, rel]
        remote(piece, piece, s_x.at[0, 0], r_x.at[wave, rel], x_pair).wait_recv()
        tt[wave, rel * 2, YROWS:, :] = tt[wave, rel * 2, YROWS:, :] + xrecv[wave, rel].astype(F32)

    def send_d(wave, kind, d):
        start(remote(dsend.at[wave, kind, d], drecv.at[wave, kind, d], s_d.at[wave, kind, d], r_d.at[wave, kind, d], y_next[d]))

    def wait_d(wave, kind, d):
        piece = drecv.at[wave, kind, d]
        remote(piece, piece, s_d.at[0, 0, 0], r_d.at[wave, kind, d], x_pair).wait_recv()
        return drecv[wave, kind, d].astype(F32)

    halves = (slice(YROWS, YROWS + XHALF), slice(YROWS + XHALF, OUT))

    for w in range(2):
        merge(w)
        terms(w, 2, 1)
        first_y(w, 0, 1, 2, 1)
        send_x(w, 2)
        terms(w, 2, 0)
        first_y(w, 0, 0, 2, 0)
        terms(w, 1, 1)
        first_y(w, 1, 0, 1, 1)
        send_x(w, 1)
        terms(w, 3, 0)
        first_y(w, 1, 1, 3, 0)
        terms(w, 3, 1)
        send_x(w, 3)
        terms(w, 1, 0)
        terms(w, 0, 1)
        send_x(w, 0)
        terms(w, 0, 0)
    for w in range(2):
        for d, n in ((0, 2), (1, 7)):
            got = wait_y(w, 0, d)
            ysend[w, 2, d] = (tt[w, n, :YROWS, :] + got).astype(BF16)
            send_y(w, 2, d)
        wait_x(w, 2)
        for d in range(2):
            dsend[w, 0, d] = tt[w, 4, halves[d], :].astype(BF16)
            send_d(w, 0, d)
        for d, rel in ((0, 1), (1, 3)):
            wait_x(w, rel)
            dsend[w, 1, d] = tt[w, 2 * rel, halves[1 - d], :].astype(BF16)
            send_d(w, 1, d)
    for w in range(2):
        for d, rel in ((0, 1), (1, 3)):
            got = wait_d(w, 0, d)
            dsend[w, 2, d] = (tt[w, 2 * rel, halves[d], :] + got).astype(BF16)
            send_d(w, 2, d)
        full = tt[w, 1, :YROWS, :] + wait_y(w, 1, 0) + wait_y(w, 2, 1)
        psend[w] = full.astype(BF16)
        start(remote(psend.at[w], precv.at[w], s_p.at[w], r_p.at[w], x_pair))
        tt[w, 0, :YROWS, :] = tt[w, 0, :YROWS, :] + wait_y(w, 2, 0) + wait_y(w, 1, 1)
    for w in range(2):
        lanes = slice(w * 128, (w + 1) * 128)
        wait_x(w, 0)
        for d in range(2):
            out_ref[halves[d], lanes] = tt[w, 0, halves[d], :] + wait_d(w, 2, d) + wait_d(w, 1, 1 - d)
        remote(precv.at[w], precv.at[w], s_p.at[0], r_p.at[w], x_pair).wait_recv()
        out_ref[:YROWS, lanes] = tt[w, 0, :YROWS, :] + precv[w].astype(F32)

    for copy in sends:
        copy.wait_send()

    def drain(i, carry):
        for d in range(2):
            remote(kvb.at[0], kvb.at[0], s_kvf.at[d, i], r_kv.at[0], partner).wait_send()
            remote(posb.at[0], posb.at[0], s_posf.at[d, i], r_pos.at[0], partner).wait_send()
        return carry

    lax.fori_loop(0, 10, drain, 0)


def on_device(query_heads, key_heads, value_heads, positions, out_weight):
    dma = pltpu.SemaphoreType.DMA
    hbm = pl.BlockSpec(memory_space=pl.ANY)
    out = pl.pallas_call(
        kernel,
        out_shape=jax.ShapeDtypeStruct((OUT, TOK), F32),
        in_specs=[hbm] * 5,
        out_specs=pl.BlockSpec(memory_space=pltpu.VMEM),
        scratch_shapes=[
            pltpu.VMEM((4 * TOK, HD), BF16),
            pltpu.VMEM((2 * TOK, HD), BF16),
            pltpu.VMEM((2 * TOK, HD), BF16),
            pltpu.VMEM((1, TOK), jnp.int32),
            pltpu.VMEM((4 * TOK, HD), F32),
            pltpu.VMEM((TOK, 4 * HD), BF16),
            pltpu.VMEM((2, 2, 256, HD), BF16),
            pltpu.VMEM((4 * NZ, QUART, 2 * HD), BF16),
            pltpu.VMEM((4 * NZ, 1, QUART), jnp.int32),
            pltpu.VMEM((4, 2, 256, HD), BF16),
            pltpu.VMEM((4, 1, TOK), jnp.int32),
            pltpu.VMEM((STEPS, STEP_KEYS, HD), BF16),
            pltpu.VMEM((STEPS, HD, STEP_KEYS), BF16),
            pltpu.VMEM((STEPS, STEP_KEYS, QUART), jnp.int32),
            pltpu.VMEM((4, 2, HD, HALF), F32),
            pltpu.VMEM((4, 2, 1, HALF), F32),
            pltpu.VMEM((4, 2, 8, HALF), F32),
            pltpu.VMEM((3, 2, HD, HALF), BF16),
            pltpu.VMEM((3, 2, 1, HALF), F32),
            pltpu.VMEM((2, 2, 2, HD, HALF), BF16),
            pltpu.VMEM((2, 2, 2, 1, HALF), F32),
            pltpu.VMEM((2, 4 * HD, 128), BF16),
            pltpu.VMEM((4 * HD, 8 * OUT), BF16),
            pltpu.VMEM((8 * OUT, 4 * HD), BF16),
            pltpu.VMEM((2, 8, OUT, 128), F32),
            pltpu.VMEM((2, 3, 2, YROWS, 128), BF16),
            pltpu.VMEM((2, 3, 2, YROWS, 128), BF16),
            pltpu.VMEM((2, 4, XROWS, 128), BF16),
            pltpu.VMEM((2, 4, XROWS, 128), BF16),
            pltpu.VMEM((2, 3, 2, XHALF, 128), BF16),
            pltpu.VMEM((2, 3, 2, XHALF, 128), BF16),
            pltpu.VMEM((2, YROWS, 128), BF16),
            pltpu.VMEM((2, YROWS, 128), BF16),
            dma((2, 4)), dma((2, 10)), dma((2, 4)), dma((2, 10)), dma((2,)), dma((2,)),
            dma((3,)), dma((3,)), dma((3, 2)), dma((3, 2)),
            dma((2, 3, 2)), dma((2, 4)), dma((2, 3, 2)), dma((2,)),
            dma((4 * NZ,)), dma((4 * NZ,)), dma((4,)), dma((4,)), dma((2, 2, 2)), dma((2, 2, 2)),
            dma((2, 3, 2)), dma((2, 4)), dma((2, 3, 2)), dma((2,)), dma((5,)),
        ],
        compiler_params=pltpu.CompilerParams(
            collective_id=0, has_side_effects=True, vmem_limit_bytes=60 * 1024 * 1024
        ),
        cost_estimate=pl.CostEstimate(flops=6_000_000_000, bytes_accessed=6_000_000, transcendentals=8_000_000),
    )(
        query_heads.reshape(4 * TOK, HD), key_heads.reshape(2 * TOK, HD), value_heads.reshape(2 * TOK, HD),
        positions.reshape(1, TOK), out_weight,
    )
    return out.astype(BF16).T


def solution(mesh):
    return jax.shard_map(
        on_device,
        mesh=mesh,
        in_specs=(
            P("ctx", "head", None),
            P("ctx", "head", None),
            P("ctx", "head", None),
            P("ctx"),
            P("head", None),
        ),
        out_specs=P("ctx", "head"),
        check_vma=False,
    )
```

```python
import jax
import jax.numpy as jnp
from jax import lax
from jax.experimental import pallas as pl
from jax.experimental.pallas import tpu as pltpu
from jax.sharding import PartitionSpec as P

MESH = pl.DeviceIdType.MESH
NEG_BIG = -1e30
LOG2E = 1.4426950408889634
SCALE = LOG2E / 12.0
NZ = 8
TOK = 256
QUART = 128
HD = 128
STEPS = NZ
STEP_KEYS = 512
HALF = 256
OUT = 576
YROWS = 288
XROWS = OUT - YROWS
XHALF = XROWS // 2
F32 = jnp.float32
BF16 = jnp.bfloat16


def kernel(
    q_hbm, k_hbm, v_hbm, pos_hbm, w_hbm, out_ref,
    q_ref, k_ref, v_ref, pos_ref, wide, kvs, qs, kvb, posb, qb, qpos, kb, vtb, pkb, acc, mrun, lrun,
    stage, lstage, attp, lsep, att, w_ref, wt,
    tt, ysend, yrecv, xsend, xrecv, dsend, drecv, psend, precv,
    s_kv1, s_kvf, s_pos1, s_posf, s_loc, s_locp, s_q, s_qp, s_o, s_l,
    s_y, s_x, s_d, s_p,
    r_kv, r_pos, r_q, r_qp, r_o, r_l, r_y, r_x, r_d, r_p, in_sem,
):
    ctx, head = lax.axis_index("ctx"), lax.axis_index("head")
    core, xh, z = ctx % 2, (ctx // 2) % 2, ctx // 4
    y, xl = head // 2, head % 2
    other = 1 - core

    def at(zz, xx, cc):
        return ((zz * 2 + xx) * 2 + cc, head)

    z_up, z_down = (z + 1) % NZ, (z + NZ - 1) % NZ
    partner = at(z, xh, other)
    y_next = ((ctx, ((y + 1) % 4) * 2 + xl), (ctx, ((y + 3) % 4) * 2 + xl))
    x_pair = (ctx, y * 2 + 1 - xl)
    peers = [partner, y_next[0], y_next[1], x_pair]
    for cc in range(2):
        peers += [at(z_up, xh, cc), at(z_down, xh, cc), at(z, 1 - xh, cc)]
    barrier = pltpu.get_barrier_semaphore()
    for peer in peers:
        pl.semaphore_signal(barrier, inc=1, device_id=peer, device_id_type=MESH)

    loads = []
    for n, (src, dst) in enumerate(((k_hbm, k_ref), (v_hbm, v_ref), (pos_hbm, pos_ref), (q_hbm, q_ref), (w_hbm, w_ref))):
        loads.append(pltpu.make_async_copy(src, dst, in_sem.at[n]))
        loads[n].start()

    for n, ref in enumerate((k_ref, v_ref)):
        loads[n].wait()
        wide[n * 512:(n + 1) * 512, :] = ref[...].astype(F32)
        for h in range(2):
            lo = h * 256 + n * HD
            kvs[:, lo:lo + HD] = wide[pl.ds(n * 512 + h, TOK, stride=2), :].astype(BF16)
    loads[2].wait()

    def remote(src, dst, ssem, rsem, dev):
        return pltpu.make_async_remote_copy(
            src_ref=src, dst_ref=dst, send_sem=ssem, recv_sem=rsem,
            device_id=dev, device_id_type=MESH,
        )

    pl.semaphore_wait(barrier, len(peers))

    sends = []

    def start(copy):
        copy.start()
        sends.append(copy)

    def kv_own(j, h):
        lane = pl.multiple_of(h * 256, 256)
        return kvs.at[pl.ds(j * QUART, QUART), pl.ds(lane, 256)]

    def pos_own(j):
        return pos_ref.at[:, pl.ds(j * QUART, QUART)]

    for n in range(4):
        for d, zz in enumerate((z_up, z_down)):
            j = n // 2 if d == 0 else 1 - n // 2
            h = core if n % 2 == 0 else other
            slot = z * 4 + core * 2 + j
            start(remote(kv_own(j, h), kvb.at[slot], s_kv1.at[d, n], r_kv.at[slot], at(zz, xh, h)))
            start(remote(pos_own(j), posb.at[slot], s_pos1.at[d, n], r_pos.at[slot], at(zz, xh, h)))
    for j in range(2):
        slot = z * 4 + core * 2 + j
        start(remote(kv_own(j, other), kvb.at[slot], s_loc.at[j], r_kv.at[slot], partner))
        start(remote(pos_own(j), posb.at[slot], s_locp.at[j], r_pos.at[slot], partner))

    loads[3].wait()
    wide[...] = q_ref[...].astype(F32)
    for h in range(2):
        for half in range(2):
            for hh in range(2):
                rows = pl.ds(half * 512 + 2 * h + hh, 128, stride=4)
                qs[h, half, hh * 128:(hh + 1) * 128, :] = wide[rows, :].astype(BF16)
    start(remote(qs.at[other], qb.at[2 + core], s_q.at[2], r_q.at[2 + core], partner))
    start(remote(pos_ref, qpos.at[2 + core], s_qp.at[2], r_qp.at[2 + core], partner))
    for h in range(2):
        dev = at(z, 1 - xh, h)
        start(remote(qs.at[h], qb.at[core], s_q.at[h], r_q.at[core], dev))
        start(remote(pos_ref, qpos.at[core], s_qp.at[h], r_qp.at[core], dev))

    qb[2 + core] = qs[core]
    qpos[2 + core] = pos_ref[...]
    mrun[...] = jnp.full(mrun.shape, NEG_BIG, F32)
    lrun[...] = jnp.zeros(lrun.shape, F32)
    acc[...] = jnp.zeros(acc.shape, F32)

    def place(step, at_quarter, kv, line):
        rows = pl.ds(pl.multiple_of(at_quarter * QUART, QUART), QUART)
        kb[step, rows, :] = kv[:, :HD]
        vtb[step, :, rows] = kv[:, HD:].T
        pkb[step, rows, :] = jnp.broadcast_to(line, (QUART, QUART)).T

    def wait_quarter(slot):
        remote(posb.at[slot], posb.at[slot], s_pos1.at[0, 0], r_pos.at[slot], partner).wait_recv()
        remote(kvb.at[slot], kvb.at[slot], s_kv1.at[0, 0], r_kv.at[slot], partner).wait_recv()

    own_lane = pl.multiple_of(core * 256, 256)
    for j in range(2):
        tokens = slice(j * QUART, (j + 1) * QUART)
        place(0, j, kvs[tokens, pl.ds(own_lane, 256)], pos_ref[:, tokens])
    def turn(i, carry):
        cols = pl.ds(pl.multiple_of(i * 128, 128), 128)
        wt[cols, :] = w_ref[:, cols].T
        return carry

    loads[4].wait()
    lax.fori_loop(0, 36, turn, 0)

    for j in range(2):
        slot = z * 4 + other * 2 + j
        wait_quarter(slot)
        place(0, 2 + j, kvb[slot], posb[slot])

    def wait_queries(g):
        remote(qb.at[g], qb.at[g], s_q.at[0], r_q.at[g], partner).wait_recv()
        remote(qpos.at[g], qpos.at[g], s_qp.at[0], r_qp.at[g], partner).wait_recv()

    wait_queries(2 + other)

    def service(i, carry):
        hop, a = i // 4 + 1, i % 4
        s = jnp.where(a % 2 == 0, core, other)
        for d in range(2):
            src_z = (z + NZ - hop) % NZ if d == 0 else (z + hop) % NZ
            j = a // 2 if d == 0 else 1 - a // 2
            slot = src_z * 4 + s * 2 + j
            dev = at(z_up if d == 0 else z_down, xh, core)
            wait_quarter(slot)

            @pl.when(i < 10)
            def _():
                remote(kvb.at[slot], kvb.at[slot], s_kvf.at[d, i], r_kv.at[slot], dev).start()
                remote(posb.at[slot], posb.at[slot], s_posf.at[d, i], r_pos.at[slot], dev).start()

            place(i // 2 + 1, (i % 2) * 2 + d, kvb[slot], posb[slot])
        return carry

    def attend(step, first):
        k = kb[step]
        vt = vtb[step]
        pk = pkb[step]
        blocks = [(first + n, half) for n in range(2) for half in range(2)]

        def scores(g, half):
            return lax.dot_general(k, qb[g, half], (((1,), (1,)), ((), ())), preferred_element_type=F32)

        every = [scores(*b) for b in blocks]
        for n, (g, half) in enumerate(blocks):
            s = every[n]
            mask = pk <= qpos[g, :, half * 128:(half + 1) * 128]
            mask = jnp.concatenate([mask, mask], axis=1)
            s = jnp.where(mask, s, NEG_BIG)
            m_old = mrun[g, half]
            m_new = jnp.maximum(m_old, jnp.max(s, axis=0, keepdims=True))
            p = jnp.exp2((s - m_new) * SCALE)
            alpha = jnp.exp2((m_old - m_new) * SCALE)
            part = jnp.sum(p.reshape(STEP_KEYS // 8, 8, HALF), axis=0)
            lrun[g, half] = lrun[g, half] * alpha + part
            mrun[g, half] = m_new
            add = jnp.dot(vt, p.astype(BF16), preferred_element_type=F32)
            acc[g, half] = acc[g, half] * alpha + add

    plan = (
        (0, 0, 2), (2, 1, 2), (4, 2, 2), (4, 0, 0), (5, 1, 0), (6, 3, 2), (6, 2, 0), (7, 3, 0),
        (8, 4, 2), (8, 4, 0), (10, 5, 2), (10, 5, 0), (12, 6, 2), (12, 6, 0), (14, 7, 0),
    )

    def planned(n, column):
        value = plan[0][column]
        for m in range(1, len(plan)):
            value = jnp.where(n == m, plan[m][column], value)
        return value

    def round_of(n, done):
        until = planned(n, 0)
        lax.fori_loop(done, until, service, 0)

        @pl.when(n == 3)
        def _():
            for g in range(2):
                wait_queries(g)

        attend(planned(n, 1), planned(n, 2))
        return until

    lax.fori_loop(0, len(plan), round_of, 0)

    def finished(g, half):
        total = jnp.sum(lrun[g, half], axis=0, keepdims=True)
        lse = mrun[g, half] * SCALE + jnp.log2(total)
        return (acc[g, half] * (1.0 / total)).astype(BF16), lse

    def give_back(n, g, half, p, dev):
        o, lse = finished(g, half)
        stage[n, half] = o
        lstage[n, half] = lse
        start(remote(stage.at[n, half], attp.at[p, core, half], s_o.at[n, half], r_o.at[p, core, half], dev))
        start(remote(lstage.at[n, half], lsep.at[p, core, half], s_l.at[n, half], r_l.at[p, core, half], dev))

    for half in range(2):
        for g in range(2):
            give_back(g, g, half, 1, at(z, 1 - xh, g))
    attend(STEPS - 1, 2)
    for half in range(2):
        give_back(2, 2 + other, half, 0, partner)
    for half in range(2):
        o, lse = finished(2 + core, half)
        attp[0, core, half] = o
        lsep[0, core, half] = lse

    def wait_part(p, h, half):
        o, lse = attp.at[p, h, half], lsep.at[p, h, half]
        remote(o, o, s_o.at[0, 0], r_o.at[p, h, half], partner).wait_recv()
        remote(lse, lse, s_l.at[0, 0], r_l.at[p, h, half], partner).wait_recv()

    def merge(half):
        wait_part(0, other, half)
        for h in range(2):
            wait_part(1, h, half)
            a, b = lsep[0, h, half], lsep[1, h, half]
            top = jnp.maximum(a, b)
            wa, wb = jnp.exp2(a - top), jnp.exp2(b - top)
            inv = 1.0 / (wa + wb)
            o = (attp[0, h, half].astype(F32) * (wa * inv) + attp[1, h, half].astype(F32) * (wb * inv)).astype(BF16)
            for hh in range(2):
                lo = (2 * h + hh) * HD
                att[half, lo:lo + HD, :] = o[:, hh * 128:(hh + 1) * 128]

    def terms(wave, rel, b):
        row = ((y + rel) % 4) * (2 * OUT) + (xl if b == 0 else 1 - xl) * OUT
        rows = pl.ds(pl.multiple_of(row, 64), OUT)
        tt[wave, rel * 2 + b] = jnp.dot(wt[rows, :], att[wave], preferred_element_type=F32)

    def send_y(wave, kind, d):
        start(remote(ysend.at[wave, kind, d], yrecv.at[wave, kind, d], s_y.at[wave, kind, d], r_y.at[wave, kind, d], y_next[d]))

    def wait_y(wave, kind, d):
        piece = yrecv.at[wave, kind, d]
        remote(piece, piece, s_y.at[0, 0, 0], r_y.at[wave, kind, d], x_pair).wait_recv()
        return yrecv[wave, kind, d].astype(F32)

    def first_y(wave, kind, d, rel, b):
        ysend[wave, kind, d] = tt[wave, rel * 2 + b, :YROWS, :].astype(BF16)
        send_y(wave, kind, d)

    def send_x(wave, rel):
        xsend[wave, rel] = tt[wave, rel * 2 + 1, YROWS:, :].astype(BF16)
        start(remote(xsend.at[wave, rel], xrecv.at[wave, rel], s_x.at[wave, rel], r_x.at[wave, rel], x_pair))

    def wait_x(wave, rel):
        piece = xrecv.at[wave, rel]
        remote(piece, piece, s_x.at[0, 0], r_x.at[wave, rel], x_pair).wait_recv()
        tt[wave, rel * 2, YROWS:, :] = tt[wave, rel * 2, YROWS:, :] + xrecv[wave, rel].astype(F32)

    def send_d(wave, kind, d):
        start(remote(dsend.at[wave, kind, d], drecv.at[wave, kind, d], s_d.at[wave, kind, d], r_d.at[wave, kind, d], y_next[d]))

    def wait_d(wave, kind, d):
        piece = drecv.at[wave, kind, d]
        remote(piece, piece, s_d.at[0, 0, 0], r_d.at[wave, kind, d], x_pair).wait_recv()
        return drecv[wave, kind, d].astype(F32)

    halves = (slice(YROWS, YROWS + XHALF), slice(YROWS + XHALF, OUT))

    for w in range(2):
        merge(w)
        terms(w, 2, 1)
        first_y(w, 0, 1, 2, 1)
        send_x(w, 2)
        terms(w, 2, 0)
        first_y(w, 0, 0, 2, 0)
        terms(w, 1, 1)
        first_y(w, 1, 0, 1, 1)
        send_x(w, 1)
        terms(w, 3, 0)
        first_y(w, 1, 1, 3, 0)
        terms(w, 3, 1)
        send_x(w, 3)
        terms(w, 1, 0)
        terms(w, 0, 1)
        send_x(w, 0)
        terms(w, 0, 0)
    for w in range(2):
        for d, n in ((0, 2), (1, 7)):
            got = wait_y(w, 0, d)
            ysend[w, 2, d] = (tt[w, n, :YROWS, :] + got).astype(BF16)
            send_y(w, 2, d)
        wait_x(w, 2)
        for d in range(2):
            dsend[w, 0, d] = tt[w, 4, halves[d], :].astype(BF16)
            send_d(w, 0, d)
        for d, rel in ((0, 1), (1, 3)):
            wait_x(w, rel)
            dsend[w, 1, d] = tt[w, 2 * rel, halves[1 - d], :].astype(BF16)
            send_d(w, 1, d)
    for w in range(2):
        for d, rel in ((0, 1), (1, 3)):
            got = wait_d(w, 0, d)
            dsend[w, 2, d] = (tt[w, 2 * rel, halves[d], :] + got).astype(BF16)
            send_d(w, 2, d)
        full = tt[w, 1, :YROWS, :] + wait_y(w, 1, 0) + wait_y(w, 2, 1)
        psend[w] = full.astype(BF16)
        start(remote(psend.at[w], precv.at[w], s_p.at[w], r_p.at[w], x_pair))
        tt[w, 0, :YROWS, :] = tt[w, 0, :YROWS, :] + wait_y(w, 2, 0) + wait_y(w, 1, 1)
    for w in range(2):
        lanes = slice(w * 128, (w + 1) * 128)
        wait_x(w, 0)
        for d in range(2):
            out_ref[halves[d], lanes] = tt[w, 0, halves[d], :] + wait_d(w, 2, d) + wait_d(w, 1, 1 - d)
        remote(precv.at[w], precv.at[w], s_p.at[0], r_p.at[w], x_pair).wait_recv()
        out_ref[:YROWS, lanes] = tt[w, 0, :YROWS, :] + precv[w].astype(F32)

    for copy in sends:
        copy.wait_send()

    def drain(i, carry):
        for d in range(2):
            remote(kvb.at[0], kvb.at[0], s_kvf.at[d, i], r_kv.at[0], partner).wait_send()
            remote(posb.at[0], posb.at[0], s_posf.at[d, i], r_pos.at[0], partner).wait_send()
        return carry

    lax.fori_loop(0, 10, drain, 0)


def on_device(query_heads, key_heads, value_heads, positions, out_weight):
    dma = pltpu.SemaphoreType.DMA
    hbm = pl.BlockSpec(memory_space=pl.ANY)
    out = pl.pallas_call(
        kernel,
        out_shape=jax.ShapeDtypeStruct((OUT, TOK), F32),
        in_specs=[hbm] * 5,
        out_specs=pl.BlockSpec(memory_space=pltpu.VMEM),
        scratch_shapes=[
            pltpu.VMEM((4 * TOK, HD), BF16),
            pltpu.VMEM((2 * TOK, HD), BF16),
            pltpu.VMEM((2 * TOK, HD), BF16),
            pltpu.VMEM((1, TOK), jnp.int32),
            pltpu.VMEM((4 * TOK, HD), F32),
            pltpu.VMEM((TOK, 4 * HD), BF16),
            pltpu.VMEM((2, 2, 256, HD), BF16),
            pltpu.VMEM((4 * NZ, QUART, 2 * HD), BF16),
            pltpu.VMEM((4 * NZ, 1, QUART), jnp.int32),
            pltpu.VMEM((4, 2, 256, HD), BF16),
            pltpu.VMEM((4, 1, TOK), jnp.int32),
            pltpu.VMEM((STEPS, STEP_KEYS, HD), BF16),
            pltpu.VMEM((STEPS, HD, STEP_KEYS), BF16),
            pltpu.VMEM((STEPS, STEP_KEYS, QUART), jnp.int32),
            pltpu.VMEM((4, 2, HD, HALF), F32),
            pltpu.VMEM((4, 2, 1, HALF), F32),
            pltpu.VMEM((4, 2, 8, HALF), F32),
            pltpu.VMEM((3, 2, HD, HALF), BF16),
            pltpu.VMEM((3, 2, 1, HALF), F32),
            pltpu.VMEM((2, 2, 2, HD, HALF), BF16),
            pltpu.VMEM((2, 2, 2, 1, HALF), F32),
            pltpu.VMEM((2, 4 * HD, 128), BF16),
            pltpu.VMEM((4 * HD, 8 * OUT), BF16),
            pltpu.VMEM((8 * OUT, 4 * HD), BF16),
            pltpu.VMEM((2, 8, OUT, 128), F32),
            pltpu.VMEM((2, 3, 2, YROWS, 128), BF16),
            pltpu.VMEM((2, 3, 2, YROWS, 128), BF16),
            pltpu.VMEM((2, 4, XROWS, 128), BF16),
            pltpu.VMEM((2, 4, XROWS, 128), BF16),
            pltpu.VMEM((2, 3, 2, XHALF, 128), BF16),
            pltpu.VMEM((2, 3, 2, XHALF, 128), BF16),
            pltpu.VMEM((2, YROWS, 128), BF16),
            pltpu.VMEM((2, YROWS, 128), BF16),
            dma((2, 4)), dma((2, 10)), dma((2, 4)), dma((2, 10)), dma((2,)), dma((2,)),
            dma((3,)), dma((3,)), dma((3, 2)), dma((3, 2)),
            dma((2, 3, 2)), dma((2, 4)), dma((2, 3, 2)), dma((2,)),
            dma((4 * NZ,)), dma((4 * NZ,)), dma((4,)), dma((4,)), dma((2, 2, 2)), dma((2, 2, 2)),
            dma((2, 3, 2)), dma((2, 4)), dma((2, 3, 2)), dma((2,)), dma((5,)),
        ],
        compiler_params=pltpu.CompilerParams(
            collective_id=0, has_side_effects=True, vmem_limit_bytes=60 * 1024 * 1024
        ),
        cost_estimate=pl.CostEstimate(flops=6_000_000_000, bytes_accessed=6_000_000, transcendentals=8_000_000),
    )(
        query_heads.reshape(4 * TOK, HD), key_heads.reshape(2 * TOK, HD), value_heads.reshape(2 * TOK, HD),
        positions.reshape(1, TOK), out_weight,
    )
    return out.astype(BF16).T


def solution(mesh):
    return jax.shard_map(
        on_device,
        mesh=mesh,
        in_specs=(
            P("ctx", "head", None),
            P("ctx", "head", None),
            P("ctx", "head", None),
            P("ctx"),
            P("head", None),
        ),
        out_specs=P("ctx", "head"),
        check_vma=False,
    )
```

```python
import jax
import jax.numpy as jnp
from jax import lax
from jax.experimental import pallas as pl
from jax.experimental.pallas import tpu as pltpu
from jax.sharding import PartitionSpec as P

MESH = pl.DeviceIdType.MESH
NEG_BIG = -1e30
LOG2E = 1.4426950408889634
SCALE = LOG2E / 12.0
NZ = 8
TOK = 256
QUART = 128
HD = 128
STEPS = NZ
STEP_KEYS = 512
HALF = 256
OUT = 576
YROWS = 288
XROWS = OUT - YROWS
XHALF = XROWS // 2
F32 = jnp.float32
BF16 = jnp.bfloat16


def kernel(
    q_hbm, k_hbm, v_hbm, pos_hbm, w_hbm, out_ref,
    q_ref, k_ref, v_ref, pos_ref, wide, kvs, qs, kvb, posb, qb, qpos, kb, vtb, pkb, acc, mrun, lrun,
    stage, lstage, attp, lsep, att, w_ref, wt,
    tt, ysend, yrecv, xsend, xrecv, dsend, drecv, psend, precv,
    s_kv1, s_kvf, s_pos1, s_posf, s_loc, s_locp, s_q, s_qp, s_o, s_l,
    s_y, s_x, s_d, s_p,
    r_kv, r_pos, r_q, r_qp, r_o, r_l, r_y, r_x, r_d, r_p, in_sem,
):
    ctx, head = lax.axis_index("ctx"), lax.axis_index("head")
    core, xh, z = ctx % 2, (ctx // 2) % 2, ctx // 4
    y, xl = head // 2, head % 2
    other = 1 - core

    def at(zz, xx, cc):
        return ((zz * 2 + xx) * 2 + cc, head)

    z_up, z_down = (z + 1) % NZ, (z + NZ - 1) % NZ
    partner = at(z, xh, other)
    y_next = ((ctx, ((y + 1) % 4) * 2 + xl), (ctx, ((y + 3) % 4) * 2 + xl))
    x_pair = (ctx, y * 2 + 1 - xl)
    peers = [partner, y_next[0], y_next[1], x_pair]
    for cc in range(2):
        peers += [at(z_up, xh, cc), at(z_down, xh, cc), at(z, 1 - xh, cc)]
    barrier = pltpu.get_barrier_semaphore()
    for peer in peers:
        pl.semaphore_signal(barrier, inc=1, device_id=peer, device_id_type=MESH)

    loads = []
    for n, (src, dst) in enumerate(((k_hbm, k_ref), (v_hbm, v_ref), (pos_hbm, pos_ref), (q_hbm, q_ref), (w_hbm, w_ref))):
        loads.append(pltpu.make_async_copy(src, dst, in_sem.at[n]))
        loads[n].start()

    for n, ref in enumerate((k_ref, v_ref)):
        loads[n].wait()
        wide[n * 512:(n + 1) * 512, :] = ref[...].astype(F32)
        for h in range(2):
            lo = h * 256 + n * HD
            kvs[:, lo:lo + HD] = wide[pl.ds(n * 512 + h, TOK, stride=2), :].astype(BF16)
    loads[2].wait()

    def remote(src, dst, ssem, rsem, dev):
        return pltpu.make_async_remote_copy(
            src_ref=src, dst_ref=dst, send_sem=ssem, recv_sem=rsem,
            device_id=dev, device_id_type=MESH,
        )

    pl.semaphore_wait(barrier, len(peers))

    sends = []

    def start(copy):
        copy.start()
        sends.append(copy)

    def kv_own(j, h):
        lane = pl.multiple_of(h * 256, 256)
        return kvs.at[pl.ds(j * QUART, QUART), pl.ds(lane, 256)]

    def pos_own(j):
        return pos_ref.at[:, pl.ds(j * QUART, QUART)]

    for n in range(4):
        for d, zz in enumerate((z_up, z_down)):
            j = n // 2 if d == 0 else 1 - n // 2
            h = core if n % 2 == 0 else other
            slot = z * 4 + core * 2 + j
            start(remote(kv_own(j, h), kvb.at[slot], s_kv1.at[d, n], r_kv.at[slot], at(zz, xh, h)))
            start(remote(pos_own(j), posb.at[slot], s_pos1.at[d, n], r_pos.at[slot], at(zz, xh, h)))
    for j in range(2):
        slot = z * 4 + core * 2 + j
        start(remote(kv_own(j, other), kvb.at[slot], s_loc.at[j], r_kv.at[slot], partner))
        start(remote(pos_own(j), posb.at[slot], s_locp.at[j], r_pos.at[slot], partner))

    loads[3].wait()
    wide[...] = q_ref[...].astype(F32)
    for h in range(2):
        for half in range(2):
            for hh in range(2):
                rows = pl.ds(half * 512 + 2 * h + hh, 128, stride=4)
                qs[h, half, hh * 128:(hh + 1) * 128, :] = wide[rows, :].astype(BF16)
    start(remote(qs.at[other], qb.at[2 + core], s_q.at[2], r_q.at[2 + core], partner))
    start(remote(pos_ref, qpos.at[2 + core], s_qp.at[2], r_qp.at[2 + core], partner))
    for h in range(2):
        dev = at(z, 1 - xh, h)
        start(remote(qs.at[h], qb.at[core], s_q.at[h], r_q.at[core], dev))
        start(remote(pos_ref, qpos.at[core], s_qp.at[h], r_qp.at[core], dev))

    qb[2 + core] = qs[core]
    qpos[2 + core] = pos_ref[...]
    mrun[...] = jnp.full(mrun.shape, NEG_BIG, F32)
    lrun[...] = jnp.zeros(lrun.shape, F32)
    acc[...] = jnp.zeros(acc.shape, F32)

    def place(step, at_quarter, kv, line):
        rows = pl.ds(pl.multiple_of(at_quarter * QUART, QUART), QUART)
        kb[step, rows, :] = kv[:, :HD]
        vtb[step, :, rows] = kv[:, HD:].T
        pkb[step, rows, :] = jnp.broadcast_to(line, (QUART, QUART)).T

    def wait_quarter(slot):
        remote(posb.at[slot], posb.at[slot], s_pos1.at[0, 0], r_pos.at[slot], partner).wait_recv()
        remote(kvb.at[slot], kvb.at[slot], s_kv1.at[0, 0], r_kv.at[slot], partner).wait_recv()

    own_lane = pl.multiple_of(core * 256, 256)
    for j in range(2):
        tokens = slice(j * QUART, (j + 1) * QUART)
        place(0, j, kvs[tokens, pl.ds(own_lane, 256)], pos_ref[:, tokens])
    def turn(i, carry):
        cols = pl.ds(pl.multiple_of(i * 128, 128), 128)
        wt[cols, :] = w_ref[:, cols].T
        return carry

    loads[4].wait()
    lax.fori_loop(0, 36, turn, 0)

    for j in range(2):
        slot = z * 4 + other * 2 + j
        wait_quarter(slot)
        place(0, 2 + j, kvb[slot], posb[slot])

    def wait_queries(g):
        remote(qb.at[g], qb.at[g], s_q.at[0], r_q.at[g], partner).wait_recv()
        remote(qpos.at[g], qpos.at[g], s_qp.at[0], r_qp.at[g], partner).wait_recv()

    wait_queries(2 + other)

    def service(i, carry):
        hop, a = i // 4 + 1, i % 4
        s = jnp.where(a % 2 == 0, core, other)
        for d in range(2):
            src_z = (z + NZ - hop) % NZ if d == 0 else (z + hop) % NZ
            j = a // 2 if d == 0 else 1 - a // 2
            slot = src_z * 4 + s * 2 + j
            dev = at(z_up if d == 0 else z_down, xh, core)
            wait_quarter(slot)

            @pl.when(i < 10)
            def _():
                remote(kvb.at[slot], kvb.at[slot], s_kvf.at[d, i], r_kv.at[slot], dev).start()
                remote(posb.at[slot], posb.at[slot], s_posf.at[d, i], r_pos.at[slot], dev).start()

            place(i // 2 + 1, (i % 2) * 2 + d, kvb[slot], posb[slot])
        return carry

    def attend(step, first, start_key=0, keys=STEP_KEYS, token_halves=(0, 1)):
        within = slice(start_key, start_key + keys)
        k = kb[step, within, :]
        vt = vtb[step, :, within]
        pk = pkb[step, within, :]
        blocks = [(first + n, half) for n in range(2) for half in token_halves]

        def scores(g, half):
            return lax.dot_general(k, qb[g, half], (((1,), (1,)), ((), ())), preferred_element_type=F32)

        every = [scores(*b) for b in blocks]
        for n, (g, half) in enumerate(blocks):
            s = every[n]
            mask = pk <= qpos[g, :, half * 128:(half + 1) * 128]
            mask = jnp.concatenate([mask, mask], axis=1)
            s = jnp.where(mask, s, NEG_BIG)
            m_old = mrun[g, half]
            m_new = jnp.maximum(m_old, jnp.max(s, axis=0, keepdims=True))
            p = jnp.exp2((s - m_new) * SCALE)
            alpha = jnp.exp2((m_old - m_new) * SCALE)
            part = jnp.sum(p.reshape(keys // 8, 8, HALF), axis=0)
            lrun[g, half] = lrun[g, half] * alpha + part
            mrun[g, half] = m_new
            add = jnp.dot(vt, p.astype(BF16), preferred_element_type=F32)
            acc[g, half] = acc[g, half] * alpha + add

    plan = (
        (0, 0, 2), (2, 1, 2), (4, 2, 2), (4, 0, 0), (5, 1, 0), (6, 3, 2), (6, 2, 0), (7, 3, 0),
        (8, 4, 2), (8, 4, 0), (10, 5, 2), (10, 5, 0), (12, 6, 2), (12, 6, 0),
    )

    def planned(n, column):
        value = plan[0][column]
        for m in range(1, len(plan)):
            value = jnp.where(n == m, plan[m][column], value)
        return value

    def round_of(n, done):
        until = planned(n, 0)
        lax.fori_loop(done, until, service, 0)

        @pl.when(n == 3)
        def _():
            for g in range(2):
                wait_queries(g)

        attend(planned(n, 1), planned(n, 2))
        return until

    lax.fori_loop(0, len(plan), round_of, 0)

    def finished(g, half):
        total = jnp.sum(lrun[g, half], axis=0, keepdims=True)
        lse = mrun[g, half] * SCALE + jnp.log2(total)
        return (acc[g, half] * (1.0 / total)).astype(BF16), lse

    def give_back(n, g, half, p, dev):
        o, lse = finished(g, half)
        stage[n, half] = o
        lstage[n, half] = lse
        start(remote(stage.at[n, half], attp.at[p, core, half], s_o.at[n, half], r_o.at[p, core, half], dev))
        start(remote(lstage.at[n, half], lsep.at[p, core, half], s_l.at[n, half], r_l.at[p, core, half], dev))

    service(12, 0)
    attend(STEPS - 1, 0, 0, STEP_KEYS // 2)
    service(13, 0)
    for half in range(2):
        attend(STEPS - 1, 0, STEP_KEYS // 2, STEP_KEYS // 2, (half,))
        for g in range(2):
            give_back(g, g, half, 1, at(z, 1 - xh, g))
    attend(STEPS - 1, 2)
    for half in range(2):
        give_back(2, 2 + other, half, 0, partner)
    for half in range(2):
        o, lse = finished(2 + core, half)
        attp[0, core, half] = o
        lsep[0, core, half] = lse

    def wait_part(p, h, half):
        o, lse = attp.at[p, h, half], lsep.at[p, h, half]
        remote(o, o, s_o.at[0, 0], r_o.at[p, h, half], partner).wait_recv()
        remote(lse, lse, s_l.at[0, 0], r_l.at[p, h, half], partner).wait_recv()

    def merge(half):
        wait_part(0, other, half)
        for h in range(2):
            wait_part(1, h, half)
            a, b = lsep[0, h, half], lsep[1, h, half]
            top = jnp.maximum(a, b)
            wa, wb = jnp.exp2(a - top), jnp.exp2(b - top)
            inv = 1.0 / (wa + wb)
            o = (attp[0, h, half].astype(F32) * (wa * inv) + attp[1, h, half].astype(F32) * (wb * inv)).astype(BF16)
            for hh in range(2):
                lo = (2 * h + hh) * HD
                att[half, lo:lo + HD, :] = o[:, hh * 128:(hh + 1) * 128]

    def terms(wave, rel, b):
        row = ((y + rel) % 4) * (2 * OUT) + (xl if b == 0 else 1 - xl) * OUT
        rows = pl.ds(pl.multiple_of(row, 64), OUT)
        tt[wave, rel * 2 + b] = jnp.dot(wt[rows, :], att[wave], preferred_element_type=F32)

    def send_y(wave, kind, d):
        start(remote(ysend.at[wave, kind, d], yrecv.at[wave, kind, d], s_y.at[wave, kind, d], r_y.at[wave, kind, d], y_next[d]))

    def wait_y(wave, kind, d):
        piece = yrecv.at[wave, kind, d]
        remote(piece, piece, s_y.at[0, 0, 0], r_y.at[wave, kind, d], x_pair).wait_recv()
        return yrecv[wave, kind, d].astype(F32)

    def first_y(wave, kind, d, rel, b):
        ysend[wave, kind, d] = tt[wave, rel * 2 + b, :YROWS, :].astype(BF16)
        send_y(wave, kind, d)

    def send_x(wave, rel):
        xsend[wave, rel] = tt[wave, rel * 2 + 1, YROWS:, :].astype(BF16)
        start(remote(xsend.at[wave, rel], xrecv.at[wave, rel], s_x.at[wave, rel], r_x.at[wave, rel], x_pair))

    def wait_x(wave, rel):
        piece = xrecv.at[wave, rel]
        remote(piece, piece, s_x.at[0, 0], r_x.at[wave, rel], x_pair).wait_recv()
        tt[wave, rel * 2, YROWS:, :] = tt[wave, rel * 2, YROWS:, :] + xrecv[wave, rel].astype(F32)

    def send_d(wave, kind, d):
        start(remote(dsend.at[wave, kind, d], drecv.at[wave, kind, d], s_d.at[wave, kind, d], r_d.at[wave, kind, d], y_next[d]))

    def wait_d(wave, kind, d):
        piece = drecv.at[wave, kind, d]
        remote(piece, piece, s_d.at[0, 0, 0], r_d.at[wave, kind, d], x_pair).wait_recv()
        return drecv[wave, kind, d].astype(F32)

    halves = (slice(YROWS, YROWS + XHALF), slice(YROWS + XHALF, OUT))

    for w in range(2):
        merge(w)
        terms(w, 2, 1)
        first_y(w, 0, 1, 2, 1)
        send_x(w, 2)
        terms(w, 2, 0)
        first_y(w, 0, 0, 2, 0)
        terms(w, 1, 1)
        first_y(w, 1, 0, 1, 1)
        send_x(w, 1)
        terms(w, 3, 0)
        first_y(w, 1, 1, 3, 0)
        terms(w, 3, 1)
        send_x(w, 3)
        terms(w, 1, 0)
        terms(w, 0, 1)
        send_x(w, 0)
        terms(w, 0, 0)
    for w in range(2):
        for d, n in ((0, 2), (1, 7)):
            got = wait_y(w, 0, d)
            ysend[w, 2, d] = (tt[w, n, :YROWS, :] + got).astype(BF16)
            send_y(w, 2, d)
        wait_x(w, 2)
        for d in range(2):
            dsend[w, 0, d] = tt[w, 4, halves[d], :].astype(BF16)
            send_d(w, 0, d)
        for d, rel in ((0, 1), (1, 3)):
            wait_x(w, rel)
            dsend[w, 1, d] = tt[w, 2 * rel, halves[1 - d], :].astype(BF16)
            send_d(w, 1, d)
    for w in range(2):
        for d, rel in ((0, 1), (1, 3)):
            got = wait_d(w, 0, d)
            dsend[w, 2, d] = (tt[w, 2 * rel, halves[d], :] + got).astype(BF16)
            send_d(w, 2, d)
        full = tt[w, 1, :YROWS, :] + wait_y(w, 1, 0) + wait_y(w, 2, 1)
        psend[w] = full.astype(BF16)
        start(remote(psend.at[w], precv.at[w], s_p.at[w], r_p.at[w], x_pair))
        tt[w, 0, :YROWS, :] = tt[w, 0, :YROWS, :] + wait_y(w, 2, 0) + wait_y(w, 1, 1)
    for w in range(2):
        lanes = slice(w * 128, (w + 1) * 128)
        wait_x(w, 0)
        for d in range(2):
            out_ref[halves[d], lanes] = tt[w, 0, halves[d], :] + wait_d(w, 2, d) + wait_d(w, 1, 1 - d)
        remote(precv.at[w], precv.at[w], s_p.at[0], r_p.at[w], x_pair).wait_recv()
        out_ref[:YROWS, lanes] = tt[w, 0, :YROWS, :] + precv[w].astype(F32)

    for copy in sends:
        copy.wait_send()

    def drain(i, carry):
        for d in range(2):
            remote(kvb.at[0], kvb.at[0], s_kvf.at[d, i], r_kv.at[0], partner).wait_send()
            remote(posb.at[0], posb.at[0], s_posf.at[d, i], r_pos.at[0], partner).wait_send()
        return carry

    lax.fori_loop(0, 10, drain, 0)


def on_device(query_heads, key_heads, value_heads, positions, out_weight):
    dma = pltpu.SemaphoreType.DMA
    hbm = pl.BlockSpec(memory_space=pl.ANY)
    out = pl.pallas_call(
        kernel,
        out_shape=jax.ShapeDtypeStruct((OUT, TOK), F32),
        in_specs=[hbm] * 5,
        out_specs=pl.BlockSpec(memory_space=pltpu.VMEM),
        scratch_shapes=[
            pltpu.VMEM((4 * TOK, HD), BF16),
            pltpu.VMEM((2 * TOK, HD), BF16),
            pltpu.VMEM((2 * TOK, HD), BF16),
            pltpu.VMEM((1, TOK), jnp.int32),
            pltpu.VMEM((4 * TOK, HD), F32),
            pltpu.VMEM((TOK, 4 * HD), BF16),
            pltpu.VMEM((2, 2, 256, HD), BF16),
            pltpu.VMEM((4 * NZ, QUART, 2 * HD), BF16),
            pltpu.VMEM((4 * NZ, 1, QUART), jnp.int32),
            pltpu.VMEM((4, 2, 256, HD), BF16),
            pltpu.VMEM((4, 1, TOK), jnp.int32),
            pltpu.VMEM((STEPS, STEP_KEYS, HD), BF16),
            pltpu.VMEM((STEPS, HD, STEP_KEYS), BF16),
            pltpu.VMEM((STEPS, STEP_KEYS, QUART), jnp.int32),
            pltpu.VMEM((4, 2, HD, HALF), F32),
            pltpu.VMEM((4, 2, 1, HALF), F32),
            pltpu.VMEM((4, 2, 8, HALF), F32),
            pltpu.VMEM((3, 2, HD, HALF), BF16),
            pltpu.VMEM((3, 2, 1, HALF), F32),
            pltpu.VMEM((2, 2, 2, HD, HALF), BF16),
            pltpu.VMEM((2, 2, 2, 1, HALF), F32),
            pltpu.VMEM((2, 4 * HD, 128), BF16),
            pltpu.VMEM((4 * HD, 8 * OUT), BF16),
            pltpu.VMEM((8 * OUT, 4 * HD), BF16),
            pltpu.VMEM((2, 8, OUT, 128), F32),
            pltpu.VMEM((2, 3, 2, YROWS, 128), BF16),
            pltpu.VMEM((2, 3, 2, YROWS, 128), BF16),
            pltpu.VMEM((2, 4, XROWS, 128), BF16),
            pltpu.VMEM((2, 4, XROWS, 128), BF16),
            pltpu.VMEM((2, 3, 2, XHALF, 128), BF16),
            pltpu.VMEM((2, 3, 2, XHALF, 128), BF16),
            pltpu.VMEM((2, YROWS, 128), BF16),
            pltpu.VMEM((2, YROWS, 128), BF16),
            dma((2, 4)), dma((2, 10)), dma((2, 4)), dma((2, 10)), dma((2,)), dma((2,)),
            dma((3,)), dma((3,)), dma((3, 2)), dma((3, 2)),
            dma((2, 3, 2)), dma((2, 4)), dma((2, 3, 2)), dma((2,)),
            dma((4 * NZ,)), dma((4 * NZ,)), dma((4,)), dma((4,)), dma((2, 2, 2)), dma((2, 2, 2)),
            dma((2, 3, 2)), dma((2, 4)), dma((2, 3, 2)), dma((2,)), dma((5,)),
        ],
        compiler_params=pltpu.CompilerParams(
            collective_id=0, has_side_effects=True, vmem_limit_bytes=60 * 1024 * 1024
        ),
        cost_estimate=pl.CostEstimate(flops=6_000_000_000, bytes_accessed=6_000_000, transcendentals=8_000_000),
    )(
        query_heads.reshape(4 * TOK, HD), key_heads.reshape(2 * TOK, HD), value_heads.reshape(2 * TOK, HD),
        positions.reshape(1, TOK), out_weight,
    )
    return out.astype(BF16).T


def solution(mesh):
    return jax.shard_map(
        on_device,
        mesh=mesh,
        in_specs=(
            P("ctx", "head", None),
            P("ctx", "head", None),
            P("ctx", "head", None),
            P("ctx"),
            P("head", None),
        ),
        out_specs=P("ctx", "head"),
        check_vma=False,
    )
```
